512 devices in a mesh: freq: 32 (over x, z), sens: 16 (over y, core).
Axes of the slice: x: 4, y: 8, z: 8, core: 2. Of those that a mesh axis runs over, the one named last changes fastest.
Arguments:
- samples: bfloat16 [512, 640, 420], P('freq', 'sens'), may hold values from -6 to 6
- response_tiles: bfloat16 [448, 2, 640, 21], P('freq', None, 'sens'), may hold values from -0.25 to 0.25
- slot_sensor: int32 [640], P('sens'), may hold values from -1 to 599, as said below
- sensor_noise: float32 [600], replicated, may hold values from 0.02 to 5
- advance_offset: int32 [21], replicated, may hold values from 0 to 419
Outputs:
- outlook_values: bfloat16 [512, 21, 420], P('freq')
- noise_spread: float32 [21], replicated
The draws below stay inside these ranges and needn't reach their ends.
Inputs may be any that keep to these rules, and one draw needn't show every extreme that they name: `slot_sensor`: every sensor number appears in exactly one slot; the other 40 slots hold -1.
All inputs are finite; a program needn't handle non-finite values.
Results may differ from the reference program's by a relative error of at most 0.0055.
Values may be sent and summed in bfloat16 or wider, within the bound.
No kernel may reach another device: no remote copies, remote signals or barrier semaphores. Data moves between devices by JAX's collectives and lax.ppermute only.
A program may use at most 64 MiB of HBM per device.

```python
import math
import jax
import jax.numpy as jnp
from jax import lax

TARGET_PLACES = 21
PROBE_COUNT = 600
HORIZON_LENGTH = 420
KEPT_HARMONICS = 448
POSTERIOR_COUNT = 512
PROBE_POSITIONS = 640
N_FREQ = 32


def draw_slot_sensor(key, part):
    ordering = jax.random.permutation(key, PROBE_POSITIONS).astype(jnp.int32)
    return jnp.where(ordering < PROBE_COUNT, ordering, -1).astype(jnp.int32)


def place_ends(drawn, rng, least, largest):
    spot = [jax.random.randint(jax.random.fold_in(rng, axis), (), 0, length) for axis, length in enumerate(drawn.shape)]
    main_axis = drawn.shape.index(max(drawn.shape))
    beside = spot[:main_axis] + [(spot[main_axis] + 1) % drawn.shape[main_axis]] + spot[main_axis + 1:]
    return drawn.at[tuple(spot)].set(least).at[tuple(beside)].set(largest)


def block_scale(own_key, dims, pieces, low, high):
    def one(position, blocks):
        draws = jax.random.uniform(jax.random.fold_in(jax.random.fold_in(own_key, 6), position), (blocks,), jnp.float32, low / len(pieces), high / len(pieces))
        return jnp.repeat(jnp.exp(draws), dims[position] // blocks).reshape((-1,) + (1,) * (len(dims) - position - 1))

    level = one(*pieces[0])
    for cut in pieces[1:]:
        level = level * one(*cut)
    return level


def noise(own_key, shape, spread, bound, shards=(), held_as=jnp.bfloat16):
    gain = block_scale(own_key, shape, shards, -0.22, 0.18) if shards else 1.0
    array = jax.random.normal(own_key, shape, jnp.float32) * spread * gain
    return jnp.minimum(jnp.maximum(array, -bound), bound).astype(held_as)


def setup_inputs(seed: int = 0) -> dict:
    splits = jax.random.split(jax.random.key(seed), 6)
    return {
        "samples": noise(splits[0], (POSTERIOR_COUNT, PROBE_POSITIONS, HORIZON_LENGTH), 1.0, 6.0, ((0, 32), (1, 16))),
        "response_tiles": noise(splits[1], (KEPT_HARMONICS, 2, PROBE_POSITIONS, TARGET_PLACES), (PROBE_COUNT * HORIZON_LENGTH // KEPT_HARMONICS) ** -0.5, 0.25, ((0, 32), (2, 16))),
        "slot_sensor": draw_slot_sensor(jax.random.fold_in(splits[5], 71), 0),
        "sensor_noise": jnp.clip(jnp.exp(jax.random.uniform(splits[3], (PROBE_COUNT,), jnp.float32, math.log(0.02), math.log(5.0))), 0.02, 5.0),
        "advance_offset": place_ends(jax.random.randint(splits[4], (TARGET_PLACES,), 0, HORIZON_LENGTH), jax.random.fold_in(splits[4], 1), 0, HORIZON_LENGTH - 1).astype(jnp.int32),
    }


def angles(first_bin, bin_count, period, factor):
    bin_index = first_bin + lax.iota(jnp.int32, bin_count)
    turn_count = (bin_index[:, None] * factor[None, :]) % period
    return turn_count.astype(jnp.float32) * (2.0 * math.pi / period)


def forward_table(bin_count, step_count, period):
    phase_angle = angles(0, bin_count, period, lax.iota(jnp.int32, step_count))
    return jnp.stack([jnp.cos(phase_angle), -jnp.sin(phase_angle)]).astype(jnp.bfloat16)


def inverse_table(bin_count, step_count, period):
    bin_index = lax.iota(jnp.int32, bin_count)
    weight = jnp.where(bin_index == 0, 1.0, 2.0).astype(jnp.float32) / period
    phase_angle = angles(0, bin_count, period, lax.iota(jnp.int32, step_count))
    return jnp.stack([weight[:, None] * jnp.cos(phase_angle), -weight[:, None] * jnp.sin(phase_angle)])


def reference(samples, response_tiles, slot_sensor, sensor_noise, advance_offset):
    period = 2 * KEPT_HARMONICS
    highest = lax.Precision.HIGHEST
    live_slot = (slot_sensor >= 0).astype(jnp.bfloat16)
    blocks = response_tiles * live_slot[None, None, :, None]
    wide = blocks.astype(jnp.float32)
    sensor_ids = lax.iota(jnp.int32, PROBE_COUNT)
    slot_noise = jnp.sum(jnp.where(slot_sensor[:, None] == sensor_ids[None, :], sensor_noise[None, :], jnp.float32(0.0)), axis=1)
    power = wide[:, 0] * wide[:, 0] + wide[:, 1] * wide[:, 1]
    bin_index = lax.iota(jnp.int32, KEPT_HARMONICS)
    bin_weight = jnp.where(bin_index == 0, 1.0, 2.0).astype(jnp.float32) / period
    per_bin = jnp.einsum("ksq,s->kq", power, slot_noise, precision=highest)
    noise_spread = jnp.dot(bin_weight, per_bin, precision=highest)

    forward_flat = forward_table(KEPT_HARMONICS, HORIZON_LENGTH, period).reshape(2 * KEPT_HARMONICS, HORIZON_LENGTH)
    backward = inverse_table(KEPT_HARMONICS, HORIZON_LENGTH, period).astype(jnp.float32)
    block_real = wide[:, 0]
    block_imag = wide[:, 1]
    twiddle = angles(0, KEPT_HARMONICS, period, advance_offset)
    cosine = jnp.cos(twiddle)[:, :, None]
    sine_part = jnp.sin(twiddle)[:, :, None]

    def product(left, right):
        return jnp.einsum("krs,ksq->kqr", left, right, precision=highest)

    def single_block(sample_block):
        row_count = sample_block.shape[0]
        flat_out = jnp.dot(sample_block.reshape(row_count * PROBE_POSITIONS, HORIZON_LENGTH), forward_flat.T, preferred_element_type=jnp.float32)
        spectra = flat_out.reshape(row_count, PROBE_POSITIONS, 2, KEPT_HARMONICS).transpose(2, 3, 0, 1).astype(jnp.bfloat16)
        spec_real = spectra[0].astype(jnp.float32)
        spec_imag = spectra[1].astype(jnp.float32)
        real_part = product(spec_real, block_real) - product(spec_imag, block_imag)
        imag_part = product(spec_real, block_imag) + product(spec_imag, block_real)
        shifted = jnp.stack([real_part * cosine - imag_part * sine_part, real_part * sine_part + imag_part * cosine])
        return jnp.einsum("ckqr,ckt->rqt", shifted, backward, precision=highest).astype(jnp.bfloat16)

    estimate_tiles = lax.map(single_block, samples.reshape(N_FREQ, POSTERIOR_COUNT // N_FREQ, PROBE_POSITIONS, HORIZON_LENGTH))
    outlook_values = estimate_tiles.reshape(POSTERIOR_COUNT, TARGET_PLACES, HORIZON_LENGTH)
    return (outlook_values, noise_spread)
```

```python
import math

import jax
import jax.numpy as jnp
import numpy as np
from jax import lax
from jax.sharding import Mesh
from jax.sharding import PartitionSpec as P

KEPT = 448
PERIOD = 2 * KEPT
X, Z, Y, C = "freq_0", "freq_1", "sens_0", "sens_1"
FREQ = (X, Z)
SENS = (Y, C)


def turns(bins, steps):
    k = np.arange(bins)[:, None]
    t = np.arange(steps)[None, :]
    return ((k * t) % PERIOD) * (2.0 * np.pi / PERIOD)


def forward_np(steps):
    a = turns(KEPT, steps)
    return np.stack([np.cos(a), -np.sin(a)])


def inverse_np(steps):
    a = turns(KEPT, steps)
    w = np.where(np.arange(KEPT) == 0, 1.0, 2.0)[:, None] / PERIOD
    return np.stack([w * np.cos(a), -w * np.sin(a)])


def share(array, axis):
    n = lax.axis_size(axis)
    return lax.all_to_all(
        jnp.broadcast_to(array[None], (n, *array.shape)), axis, 0, 0, tiled=True
    )


def three(v):
    hi = v.astype(jnp.bfloat16)
    r = v - hi.astype(jnp.float32)
    mid = r.astype(jnp.bfloat16)
    lo = (r - mid.astype(jnp.float32)).astype(jnp.bfloat16)
    return jnp.stack([hi, mid, lo])


def on_device(samples, response, slot_sensor, sensor_noise, advance_offset):
    f32, bf16 = jnp.float32, jnp.bfloat16
    rows, slots, steps = samples.shape
    bins, _, _, sites = response.shape
    first_bin = lax.axis_index(FREQ) * bins
    live = slot_sensor >= 0
    blocks = jnp.where(live[None, None, :, None], response, 0)
    ids = lax.iota(jnp.int32, sensor_noise.shape[0])
    slot_noise = jnp.sum(
        jnp.where(slot_sensor[:, None] == ids[None, :], sensor_noise[None, :], 0.0), axis=1
    )
    wide = blocks.astype(f32)
    k_own = first_bin + lax.iota(jnp.int32, bins)
    weight = jnp.where(k_own == 0, 1.0, 2.0).astype(f32) / PERIOD
    noise_own = jnp.sum(
        wide * wide * slot_noise[None, None, :, None] * weight[:, None, None, None], axis=(0, 1, 2)
    )
    flat = blocks.transpose(3, 0, 1, 2).reshape(sites, bins * 2 * slots)
    tiles = -(-bins * 2 * slots // 128)
    flat = jnp.pad(flat, ((0, 0), (0, tiles * 128 - flat.shape[1])))
    flat = flat.reshape(sites, tiles, 128).transpose(1, 0, 2).reshape(tiles * sites, 128)
    extra = jnp.pad(three(noise_own), ((0, 0), (0, 128 - sites)))
    payload = jnp.concatenate([flat, extra], axis=0)
    gathered = share(share(payload, Z), X)
    gathered = gathered.reshape(-1, tiles * sites + 3, 128)

    forward = jnp.asarray(forward_np(steps), bf16)
    spectra = jnp.einsum("rst,ckt->ckrs", samples, forward, preferred_element_type=f32)
    spectra = spectra.astype(bf16)
    sre, sim = spectra[0], spectra[1]
    left = jnp.stack(
        [jnp.concatenate([sre, -sim], axis=2), jnp.concatenate([sim, sre], axis=2)], axis=1
    ).reshape(KEPT, 2 * rows, 2 * slots)

    noise_freq = jnp.sum(gathered[:, tiles * sites :, :sites].astype(f32), axis=(0, 1))
    blk = gathered[:, : tiles * sites].reshape(-1, tiles, sites, 128).transpose(0, 2, 1, 3)
    blk = blk.reshape(-1, sites, tiles * 128)[:, :, : bins * 2 * slots]
    blk = blk.reshape(-1, sites, bins, 2 * slots).transpose(0, 2, 1, 3)
    blk = blk.reshape(KEPT, sites, 2 * slots)
    zc = jnp.einsum("kns,kqs->knq", left, blk, preferred_element_type=f32)
    zc = zc.reshape(KEPT, 2, rows, sites)
    k_all = lax.iota(jnp.int32, KEPT)
    turn = (k_all[:, None] * advance_offset[None, :]) % PERIOD
    ang = turn.astype(f32) * (2.0 * math.pi / PERIOD)
    cos, sin = jnp.cos(ang)[:, None, :], jnp.sin(ang)[:, None, :]
    z0, z1 = zc[:, 0], zc[:, 1]
    shifted = jnp.stack([z0 * cos - z1 * sin, z0 * sin + z1 * cos]).astype(bf16)
    backward = jnp.asarray(inverse_np(steps), bf16)
    part = jnp.einsum("ckrq,ckt->rqt", shifted, backward, preferred_element_type=f32)
    lanes = -(-(steps + 3) // 128) * 128
    tail = three(noise_freq).T
    tail = jnp.broadcast_to(tail[None], (rows, sites, 3))
    piece = jnp.concatenate(
        [part.astype(bf16), tail, jnp.zeros((rows, sites, lanes - steps - 3), bf16)], axis=2
    )
    got = lax.all_to_all(piece, SENS, 0, 0, tiled=True)
    total = jnp.sum(got.astype(f32), axis=0)
    noise_spread = jnp.sum(total[:, steps : steps + 3], axis=1)
    own = total.astype(bf16)
    outlook = share(own, SENS)[:, :, :steps]
    return outlook, noise_spread


def solution(mesh):
    torus = Mesh(mesh.devices.reshape(4, 8, 8, 2), (X, Z, Y, C))
    return jax.shard_map(
        on_device,
        mesh=torus,
        in_specs=(P(FREQ, SENS, None), P(FREQ, None, SENS, None), P(SENS), P(), P()),
        out_specs=(P(FREQ, None, None), P()),
        check_vma=False,
    )
```

```python
import functools
import math

import jax
import jax.numpy as jnp
import numpy as np
from jax import lax
from jax.experimental import pallas as pl
from jax.experimental.pallas import tpu as pltpu
from jax.sharding import Mesh
from jax.sharding import PartitionSpec as P

KEPT = 448
PERIOD = 2 * KEPT
BINS, SLOTS, SITES, STEPS, ROWS = 14, 40, 21, 420, 16
SOURCES = KEPT // BINS
CHUNKS, HALVES = 6, 5
DEPTH = HALVES * SLOTS
TALL = SOURCES * CHUNKS * 8
WIDE = 512
X, Z, Y, C = "freq_0", "freq_1", "sens_0", "sens_1"
FREQ = (X, Z)
SENS = (Y, C)
f32, bf16 = jnp.float32, jnp.bfloat16
PLAIN = (((1,), (0,)), ((), ()))


def base_table():
    k = np.arange(KEPT)[:, None]
    t = np.arange(STEPS)[None, :]
    a = ((k * t) % PERIOD) * (2.0 * np.pi / PERIOD)
    return np.stack([np.cos(a), -np.sin(a)], axis=1)


def chunk_rows(table):
    table = table.reshape(SOURCES, BINS, 2, STEPS)
    table = jnp.pad(table, ((0, 0), (0, 2), (0, 0), (0, WIDE - STEPS)))
    parts = [table[:, 5 * g // 2 : 5 * g // 2 + 4] for g in range(CHUNKS)]
    return jnp.stack(parts, axis=1)


def chunk_mask():
    mask = np.zeros((CHUNKS, 8, 256), np.float32)
    for g in range(CHUNKS):
        for h in range(HALVES):
            if 5 * g + h < 2 * BINS:
                b = (5 * g + h) // 2 - 5 * g // 2
                mask[g, 2 * b : 2 * b + 2, h * SLOTS : (h + 1) * SLOTS] = 1.0
    return mask.reshape(CHUNKS * 8, 256)


def spread_kernel(xa_ref, xb_ref, ta_ref, tb_ref, mask_ref, out_ref):
    dims = (((1,), (1,)), ((), ()))
    mask = mask_ref[...]
    halves = []
    for j in range(2):
        d = lax.dot_general(ta_ref[...], xa_ref[j], dims, preferred_element_type=f32)
        d += lax.dot_general(tb_ref[...], xb_ref[j], dims, preferred_element_type=f32)
        d = d.reshape(SOURCES, CHUNKS * 8, 256) * mask[None]
        halves.append(d.reshape(SOURCES * CHUNKS, 8, 256))
    both = jnp.concatenate(halves, axis=1).astype(bf16)
    out_ref[...] = both.reshape(SOURCES, CHUNKS, 16, 256)


def spread(samples, forward):
    rows = chunk_rows(forward)
    re, im = rows[..., 0, :], rows[..., 1, :]
    turned = jnp.stack([-im, re], axis=-2)
    even = (jnp.arange(CHUNKS) % 2 == 0)[None, :, None, None, None]
    ta = jnp.where(even, rows, turned).reshape(TALL, WIDE)
    tb = jnp.where(even, turned, rows).reshape(TALL, WIDE)
    x = jnp.pad(samples, ((0, 0), (0, 0), (0, WIDE - STEPS)))
    o = jnp.zeros_like(x)
    e = jnp.zeros((ROWS, 256 - DEPTH, WIDE), bf16)
    xa = jnp.concatenate([x, o, x, o, x, e], axis=1)
    xb = jnp.concatenate([o, x, o, x, o, e], axis=1)
    return pl.pallas_call(
        spread_kernel,
        grid=(ROWS // 2,),
        in_specs=[
            pl.BlockSpec((2, 256, WIDE), lambda p: (p, 0, 0)),
            pl.BlockSpec((2, 256, WIDE), lambda p: (p, 0, 0)),
            pl.BlockSpec((TALL, WIDE), lambda p: (0, 0)),
            pl.BlockSpec((TALL, WIDE), lambda p: (0, 0)),
            pl.BlockSpec((CHUNKS * 8, 256), lambda p: (0, 0)),
        ],
        out_specs=pl.BlockSpec((SOURCES, CHUNKS, 16, 256), lambda p: (0, 0, p, 0)),
        out_shape=jax.ShapeDtypeStruct((SOURCES, CHUNKS, 8 * ROWS, 256), bf16),
        cost_estimate=pl.CostEstimate(
            flops=4 * TALL * WIDE * 256 * ROWS, transcendentals=0, bytes_accessed=30_000_000
        ),
        name="spread",
    )(xa, xb, ta, tb, jnp.asarray(chunk_mask()))


BLOCK = 8


def finish_kernel(left_ref, gath_ref, inv_ref, tail_ref, out_ref, z_ref):
    step = pl.program_id(0)
    lane = lax.broadcasted_iota(jnp.int32, (4, 8, 128), 2)
    for i in range(BLOCK):
        left = left_ref[i].reshape(CHUNKS * 8 * ROWS, 256)[:, :DEPTH]
        prod = lax.dot_general(left, gath_ref[i], PLAIN, preferred_element_type=f32)
        prod = prod.reshape(CHUNKS, 4, 4, 8, 128)
        packed = []
        for g in range(CHUNKS):
            acc = jnp.zeros((4, 8, 128), f32)
            for r in range(4):
                moved = pltpu.roll(prod[g, :, r], (32 * r - SITES * g) % 128, 2)
                acc = jnp.where((lane >= 32 * r) & (lane < 32 * r + SITES), moved, acc)
            packed.append(acc)
        start = pl.multiple_of((step * BLOCK + i) * CHUNKS * 8, 16)
        for q in range(4):
            col = jnp.concatenate([packed[g][q] for g in range(CHUNKS)], axis=0)
            z_ref[pl.ds(start, CHUNKS * 8), 128 * q : 128 * (q + 1)] = col.astype(bf16)

    @pl.when(step == SOURCES // BLOCK - 1)
    def _():
        total = lax.dot_general(inv_ref[...], z_ref[...], PLAIN, preferred_element_type=f32)
        total = total.T * (2.0 / PERIOD)
        total = total.reshape(ROWS, 32, WIDE) + tail_ref[...][None]
        out_ref[...] = total[:, :24].astype(bf16)


def finish(left, gathered, inverse, tail):
    return pl.pallas_call(
        finish_kernel,
        grid=(SOURCES // BLOCK,),
        in_specs=[
            pl.BlockSpec((BLOCK, CHUNKS, 8 * ROWS, 256), lambda p: (p, 0, 0, 0)),
            pl.BlockSpec((BLOCK, DEPTH, 128), lambda p: (p, 0, 0)),
            pl.BlockSpec((WIDE, TALL), lambda p: (0, 0)),
            pl.BlockSpec((32, WIDE), lambda p: (0, 0)),
        ],
        out_specs=pl.BlockSpec((ROWS, 24, WIDE), lambda p: (0, 0, 0)),
        out_shape=jax.ShapeDtypeStruct((ROWS, 24, WIDE), bf16),
        scratch_shapes=[pltpu.VMEM((TALL, 4 * 128), bf16)],
        name="finish",
    )(left, gathered, inverse, tail)


def inverse_of(forward):
    half = jnp.where(jnp.arange(KEPT) == 0, 0.5, 1.0).astype(bf16)
    return chunk_rows(forward * half[:, None, None]).reshape(TALL, WIDE).T


def share(array, axis):
    n = lax.axis_size(axis)
    return lax.all_to_all(
        jnp.broadcast_to(array[None], (n, *array.shape)), axis, 0, 0, tiled=True
    )


def three(v):
    hi = v.astype(bf16)
    r = v - hi.astype(f32)
    mid = r.astype(bf16)
    lo = (r - mid.astype(f32)).astype(bf16)
    return jnp.stack([hi, mid, lo])


def payload_of(response, slot_sensor, sensor_noise, advance_offset, first_bin):
    live = slot_sensor >= 0
    blocks = jnp.where(live[None, None, :, None], response, 0).astype(f32)
    ids = lax.iota(jnp.int32, sensor_noise.shape[0])
    slot_noise = jnp.sum(
        jnp.where(slot_sensor[:, None] == ids[None, :], sensor_noise[None, :], 0.0), axis=1
    )
    k_own = first_bin + lax.iota(jnp.int32, BINS)
    weight = jnp.where(k_own == 0, 1.0, 2.0).astype(f32) / PERIOD
    noise_own = jnp.sum(
        blocks * blocks * slot_noise[None, None, :, None] * weight[:, None, None, None],
        axis=(0, 1, 2),
    )
    turn = (k_own[:, None] * advance_offset[None, :]) % PERIOD
    ang = turn.astype(f32) * (2.0 * math.pi / PERIOD)
    cos, sin = jnp.cos(ang)[:, None, :], jnp.sin(ang)[:, None, :]
    re, im = blocks[:, 0], blocks[:, 1]
    turned = jnp.stack([re * cos - im * sin, re * sin + im * cos], axis=1).astype(bf16)
    half = turned.reshape(2 * BINS, SLOTS, SITES)
    half = jnp.pad(half, ((0, CHUNKS * HALVES - 2 * BINS), (0, 0), (0, 0)))
    half = half.reshape(CHUNKS, DEPTH, SITES).transpose(1, 0, 2).reshape(DEPTH, CHUNKS * SITES)
    side = jnp.pad(three(noise_own), ((0, 0), (0, 64 - SITES))).reshape(192)
    side = jnp.pad(side, (0, 8))[:, None]
    return jnp.concatenate([half, side, jnp.zeros_like(side)], axis=1)


def tail_of(gathered):
    side = jnp.sum(gathered[:, :192, 126].astype(f32), axis=0)
    noise = jnp.sum(side.reshape(3, 64), axis=0)[:SITES]
    return jnp.pad(three(noise).astype(f32), ((SITES, 8), (0, WIDE - SITES)))


def on_device(samples, response, slot_sensor, sensor_noise, advance_offset):
    first_bin = lax.axis_index(FREQ) * BINS
    forward = lax.optimization_barrier(jnp.asarray(base_table(), bf16))
    payload = payload_of(response, slot_sensor, sensor_noise, advance_offset, first_bin)
    gathered = share(share(payload, Z), X).reshape(SOURCES, DEPTH, 128)
    left = spread(samples, forward)
    piece = finish(left, gathered, inverse_of(forward), tail_of(gathered))
    got = lax.all_to_all(piece, SENS, 0, 0, tiled=True)
    total = jnp.sum(got.astype(f32), axis=0)
    noise_spread = jnp.sum(total[SITES:24, :SITES], axis=0)
    outlook = share(total.astype(bf16), SENS)[:, :SITES, :STEPS]
    return outlook, noise_spread


def solution(mesh):
    torus = Mesh(mesh.devices.reshape(4, 8, 8, 2), (X, Z, Y, C))
    return jax.shard_map(
        on_device,
        mesh=torus,
        in_specs=(P(FREQ, SENS, None), P(FREQ, None, SENS, None), P(SENS), P(), P()),
        out_specs=(P(FREQ, None, None), P()),
        check_vma=False,
    )
```

```python
import functools
import math

import jax
import jax.numpy as jnp
import numpy as np
from jax import lax
from jax.experimental import pallas as pl
from jax.experimental.pallas import tpu as pltpu
from jax.sharding import Mesh
from jax.sharding import PartitionSpec as P

KEPT = 448
PERIOD = 2 * KEPT
BINS, SLOTS, SITES, STEPS, ROWS = 14, 40, 21, 420, 16
SOURCES = KEPT // BINS
CHUNKS, HALVES = 6, 5
DEPTH = HALVES * SLOTS
TALL = SOURCES * CHUNKS * 8
WIDE = 512
X, Z, Y, C = "freq_0", "freq_1", "sens_0", "sens_1"
FREQ = (X, Z)
SENS = (Y, C)
f32, bf16 = jnp.float32, jnp.bfloat16
PLAIN = (((1,), (0,)), ((), ()))


def base_table():
    k = np.arange(KEPT)[:, None]
    t = np.arange(STEPS)[None, :]
    a = ((k * t) % PERIOD) * (2.0 * np.pi / PERIOD)
    return np.stack([np.cos(a), -np.sin(a)], axis=1)


def chunk_rows():
    table = base_table().reshape(SOURCES, BINS, 2, STEPS)
    table = np.pad(table, ((0, 0), (0, 2), (0, 0), (0, WIDE - STEPS)))
    parts = [table[:, 5 * g // 2 : 5 * g // 2 + 4] for g in range(CHUNKS)]
    return np.stack(parts, axis=1).reshape(TALL, WIDE)


def chunk_mask():
    mask = np.zeros((CHUNKS, 8, 256), np.float32)
    for g in range(CHUNKS):
        for h in range(HALVES):
            if 5 * g + h < 2 * BINS:
                b = (5 * g + h) // 2 - 5 * g // 2
                mask[g, 2 * b : 2 * b + 2, h * SLOTS : (h + 1) * SLOTS] = 1.0
    return mask.reshape(CHUNKS * 8, 256)


def spread_kernel(x_ref, table_ref, mask_ref, out_ref, inv_ref, ta_ref, tb_ref, xa_ref, xb_ref):
    dims = (((1,), (1,)), ((), ()))

    @pl.when(pl.program_id(0) == 0)
    def _():
        rows = table_ref[...]
        wide = rows.astype(f32).reshape(SOURCES, CHUNKS, 8, WIDE)
        sub = lax.broadcasted_iota(jnp.int32, wide.shape, 2)
        turned = jnp.where(sub % 2 == 0, -pltpu.roll(wide, 7, 2), pltpu.roll(wide, 1, 2))
        odd = lax.broadcasted_iota(jnp.int32, wide.shape, 1) % 2 == 1
        ta_ref[...] = jnp.where(odd, turned, wide).reshape(TALL, WIDE).astype(bf16)
        tb_ref[...] = jnp.where(odd, wide, turned).reshape(TALL, WIDE).astype(bf16)
        first = lax.broadcasted_iota(jnp.int32, (TALL, WIDE), 0) < 2
        inv_ref[...] = (rows.astype(f32) * jnp.where(first, 0.5, 1.0)).T.astype(bf16)
        xa_ref[...] = jnp.zeros_like(xa_ref)
        xb_ref[...] = jnp.zeros_like(xb_ref)

    mask = mask_ref[...]
    halves = []
    for j in range(2):
        x = x_ref[j]
        for h in range(HALVES):
            to = xa_ref if h % 2 == 0 else xb_ref
            to[j, h * SLOTS : (h + 1) * SLOTS, :STEPS] = x
        d = lax.dot_general(ta_ref[...], xa_ref[j], dims, preferred_element_type=f32)
        d += lax.dot_general(tb_ref[...], xb_ref[j], dims, preferred_element_type=f32)
        d = d.reshape(SOURCES, CHUNKS * 8, 256) * mask[None]
        halves.append(d.reshape(SOURCES * CHUNKS, 8, 256))
    both = jnp.concatenate(halves, axis=1).astype(bf16)
    out_ref[...] = both.reshape(SOURCES, CHUNKS, 16, 256)


def spread(samples, table):
    return pl.pallas_call(
        spread_kernel,
        grid=(ROWS // 2,),
        in_specs=[
            pl.BlockSpec((2, SLOTS, STEPS), lambda p: (p, 0, 0)),
            pl.BlockSpec((TALL, WIDE), lambda p: (0, 0)),
            pl.BlockSpec((CHUNKS * 8, 256), lambda p: (0, 0)),
        ],
        out_specs=[
            pl.BlockSpec((SOURCES, CHUNKS, 16, 256), lambda p: (0, 0, p, 0)),
            pl.BlockSpec((WIDE, TALL), lambda p: (0, 0)),
        ],
        out_shape=[
            jax.ShapeDtypeStruct((SOURCES, CHUNKS, 8 * ROWS, 256), bf16),
            jax.ShapeDtypeStruct((WIDE, TALL), bf16),
        ],
        scratch_shapes=[
            pltpu.VMEM((TALL, WIDE), bf16),
            pltpu.VMEM((TALL, WIDE), bf16),
            pltpu.VMEM((2, 256, WIDE), bf16),
            pltpu.VMEM((2, 256, WIDE), bf16),
        ],
        cost_estimate=pl.CostEstimate(
            flops=4 * TALL * WIDE * 256 * ROWS, transcendentals=0, bytes_accessed=30_000_000
        ),
        name="spread",
    )(samples, table, jnp.asarray(chunk_mask()))


BLOCK = 8


def finish_kernel(left_ref, gath_ref, inv_ref, tail_ref, out_ref, z_ref):
    step = pl.program_id(0)
    lane = lax.broadcasted_iota(jnp.int32, (4, 8, 128), 2)
    for i in range(BLOCK):
        left = left_ref[i].reshape(CHUNKS * 8 * ROWS, 256)[:, :DEPTH]
        prod = lax.dot_general(left, gath_ref[i], PLAIN, preferred_element_type=f32)
        prod = prod.reshape(CHUNKS, 4, 4, 8, 128)
        packed = []
        for g in range(CHUNKS):
            acc = jnp.zeros((4, 8, 128), f32)
            for r in range(4):
                moved = pltpu.roll(prod[g, :, r], (32 * r - SITES * g) % 128, 2)
                acc = jnp.where((lane >= 32 * r) & (lane < 32 * r + SITES), moved, acc)
            packed.append(acc)
        start = pl.multiple_of((step * BLOCK + i) * CHUNKS * 8, 16)
        for q in range(4):
            col = jnp.concatenate([packed[g][q] for g in range(CHUNKS)], axis=0)
            z_ref[pl.ds(start, CHUNKS * 8), 128 * q : 128 * (q + 1)] = col.astype(bf16)

    @pl.when(step == SOURCES // BLOCK - 1)
    def _():
        total = lax.dot_general(inv_ref[...], z_ref[...], PLAIN, preferred_element_type=f32)
        total = total.T * (2.0 / PERIOD)
        total = total.reshape(ROWS, 32, WIDE) + tail_ref[...][None]
        out_ref[...] = total[:, :24].astype(bf16)


def finish(left, gathered, inverse, tail):
    return pl.pallas_call(
        finish_kernel,
        grid=(SOURCES // BLOCK,),
        in_specs=[
            pl.BlockSpec((BLOCK, CHUNKS, 8 * ROWS, 256), lambda p: (p, 0, 0, 0)),
            pl.BlockSpec((BLOCK, DEPTH, 128), lambda p: (p, 0, 0)),
            pl.BlockSpec((WIDE, TALL), lambda p: (0, 0)),
            pl.BlockSpec((32, WIDE), lambda p: (0, 0)),
        ],
        out_specs=pl.BlockSpec((ROWS, 24, WIDE), lambda p: (0, 0, 0)),
        out_shape=jax.ShapeDtypeStruct((ROWS, 24, WIDE), bf16),
        scratch_shapes=[pltpu.VMEM((TALL, 4 * 128), bf16)],
        name="finish",
    )(left, gathered, inverse, tail)


def share(array, axis):
    n = lax.axis_size(axis)
    return lax.all_to_all(
        jnp.broadcast_to(array[None], (n, *array.shape)), axis, 0, 0, tiled=True
    )


def three(v):
    hi = v.astype(bf16)
    r = v - hi.astype(f32)
    mid = r.astype(bf16)
    lo = (r - mid.astype(f32)).astype(bf16)
    return jnp.stack([hi, mid, lo])


def payload_of(response, slot_sensor, sensor_noise, advance_offset, first_bin):
    live = slot_sensor >= 0
    blocks = jnp.where(live[None, None, :, None], response, 0).astype(f32)
    ids = lax.iota(jnp.int32, sensor_noise.shape[0])
    slot_noise = jnp.sum(
        jnp.where(slot_sensor[:, None] == ids[None, :], sensor_noise[None, :], 0.0), axis=1
    )
    k_own = first_bin + lax.iota(jnp.int32, BINS)
    weight = jnp.where(k_own == 0, 1.0, 2.0).astype(f32) / PERIOD
    noise_own = jnp.sum(
        blocks * blocks * slot_noise[None, None, :, None] * weight[:, None, None, None],
        axis=(0, 1, 2),
    )
    turn = (k_own[:, None] * advance_offset[None, :]) % PERIOD
    ang = turn.astype(f32) * (2.0 * math.pi / PERIOD)
    cos, sin = jnp.cos(ang)[:, None, :], jnp.sin(ang)[:, None, :]
    re, im = blocks[:, 0], blocks[:, 1]
    turned = jnp.stack([re * cos - im * sin, re * sin + im * cos], axis=1).astype(bf16)
    half = turned.reshape(2 * BINS, SLOTS, SITES)
    half = jnp.pad(half, ((0, CHUNKS * HALVES - 2 * BINS), (0, 0), (0, 0)))
    half = half.reshape(CHUNKS, DEPTH, SITES).transpose(1, 0, 2).reshape(DEPTH, CHUNKS * SITES)
    side = jnp.pad(three(noise_own), ((0, 0), (0, 64 - SITES))).reshape(192)
    side = jnp.pad(side, (0, 8))[:, None]
    return jnp.concatenate([half, side, jnp.zeros_like(side)], axis=1)


def tail_of(gathered):
    side = jnp.sum(gathered[:, :192, 126].astype(f32), axis=0)
    noise = jnp.sum(side.reshape(3, 64), axis=0)[:SITES]
    return jnp.pad(three(noise).astype(f32), ((SITES, 8), (0, WIDE - SITES)))


def on_device(samples, response, slot_sensor, sensor_noise, advance_offset):
    first_bin = lax.axis_index(FREQ) * BINS
    payload = payload_of(response, slot_sensor, sensor_noise, advance_offset, first_bin)
    gathered = share(share(payload, Z), X).reshape(SOURCES, DEPTH, 128)
    left, inverse = spread(samples, jnp.asarray(chunk_rows(), bf16))
    piece = finish(left, gathered, inverse, tail_of(gathered))
    got = lax.all_to_all(piece, SENS, 0, 0, tiled=True)
    total = jnp.sum(got.astype(f32), axis=0)
    noise_spread = jnp.sum(total[SITES:24, :SITES], axis=0)
    outlook = share(total.astype(bf16), SENS)[:, :SITES, :STEPS]
    return outlook, noise_spread


def solution(mesh):
    torus = Mesh(mesh.devices.reshape(4, 8, 8, 2), (X, Z, Y, C))
    return jax.shard_map(
        on_device,
        mesh=torus,
        in_specs=(P(FREQ, SENS, None), P(FREQ, None, SENS, None), P(SENS), P(), P()),
        out_specs=(P(FREQ, None, None), P()),
        check_vma=False,
    )
```

```python
import math

import jax
import jax.numpy as jnp
import numpy as np
from jax import lax
from jax.experimental import pallas as pl
from jax.experimental.pallas import tpu as pltpu
from jax.sharding import Mesh
from jax.sharding import PartitionSpec as P

KEPT = 448
PERIOD = 2 * KEPT
BINS, SLOTS, SITES, STEPS, ROWS = 14, 40, 21, 420, 16
SOURCES = KEPT // BINS
CHUNKS, HALVES = 6, 5
DEPTH = HALVES * SLOTS
TALL = SOURCES * CHUNKS * 8
WIDE = 512
X, Z, Y, C = "freq_0", "freq_1", "sens_0", "sens_1"
FREQ = (X, Z)
SENS = (Y, C)
f32, bf16 = jnp.float32, jnp.bfloat16
PLAIN = (((1,), (0,)), ((), ()))
TURNED = (((1,), (1,)), ((), ()))


def base_table():
    k = np.arange(KEPT)[:, None]
    t = np.arange(STEPS)[None, :]
    a = ((k * t) % PERIOD) * (2.0 * np.pi / PERIOD)
    return np.stack([np.cos(a), -np.sin(a)], axis=1)


def chunk_rows():
    table = base_table().reshape(SOURCES, BINS, 2, STEPS)
    table = np.pad(table, ((0, 0), (0, 2), (0, 0), (0, WIDE - STEPS)))
    parts = [table[:, 5 * g // 2 : 5 * g // 2 + 4] for g in range(CHUNKS)]
    return np.stack(parts, axis=1).swapaxes(2, 3).reshape(TALL, WIDE)


def chunk_masks():
    same = np.zeros((CHUNKS, 2, 4, 256), np.float32)
    swap = np.zeros((CHUNKS, 2, 4, 256), np.float32)
    for g in range(CHUNKS):
        for h in range(HALVES):
            half = 5 * g + h
            if half < 2 * BINS:
                b = half // 2 - 5 * g // 2
                lanes = slice(h * SLOTS, (h + 1) * SLOTS)
                if half % 2 == 0:
                    same[g, :, b, lanes] = 1.0
                else:
                    swap[g, 0, b, lanes] = -1.0
                    swap[g, 1, b, lanes] = 1.0
    return same.reshape(CHUNKS, 8, 256), swap.reshape(CHUNKS, 8, 256)


def spread_kernel(x_ref, live_ref, table_ref, same_ref, swap_ref, out_ref, inv_ref, x5_ref):
    @pl.when(pl.program_id(0) == 0)
    def _():
        rows = table_ref[...].astype(f32)
        place = lax.broadcasted_iota(jnp.int32, (TALL, WIDE), 0)
        inv_ref[...] = (rows * jnp.where((place == 0) | (place == 4), 0.5, 1.0)).T.astype(bf16)
        x5_ref[...] = jnp.zeros_like(x5_ref)

    halves = []
    for j in range(2):
        x = x_ref[j] * live_ref[...]
        for h in range(HALVES):
            x5_ref[j, h * SLOTS : (h + 1) * SLOTS, :STEPS] = x
        d = lax.dot_general(table_ref[...], x5_ref[j], TURNED, preferred_element_type=f32)
        d = d.reshape(SOURCES, CHUNKS, 8, 256)
        halves.append(d * same_ref[...][None] + pltpu.roll(d, 4, 2) * swap_ref[...][None])
    out_ref[...] = jnp.concatenate(halves, axis=2).astype(bf16)


def spread(samples, live):
    same, swap = chunk_masks()
    return pl.pallas_call(
        spread_kernel,
        grid=(ROWS // 2,),
        in_specs=[
            pl.BlockSpec((2, SLOTS, STEPS), lambda p: (p, 0, 0)),
            pl.BlockSpec((SLOTS, 1), lambda p: (0, 0)),
            pl.BlockSpec((TALL, WIDE), lambda p: (0, 0)),
            pl.BlockSpec((CHUNKS, 8, 256), lambda p: (0, 0, 0)),
            pl.BlockSpec((CHUNKS, 8, 256), lambda p: (0, 0, 0)),
        ],
        out_specs=[
            pl.BlockSpec((SOURCES, CHUNKS, 16, 256), lambda p: (0, 0, p, 0)),
            pl.BlockSpec((WIDE, TALL), lambda p: (0, 0)),
        ],
        out_shape=[
            jax.ShapeDtypeStruct((SOURCES, CHUNKS, 8 * ROWS, 256), bf16),
            jax.ShapeDtypeStruct((WIDE, TALL), bf16),
        ],
        scratch_shapes=[pltpu.VMEM((2, 256, WIDE), bf16)],
        cost_estimate=pl.CostEstimate(
            flops=2 * TALL * WIDE * 256 * ROWS, transcendentals=0, bytes_accessed=16_000_000
        ),
        name="spread",
    )(samples, live, jnp.asarray(chunk_rows(), bf16), jnp.asarray(same), jnp.asarray(swap))


def three(v):
    hi = v.astype(bf16).astype(f32)
    mid = (v - hi).astype(bf16).astype(f32)
    return hi, mid, v - hi - mid


BLOCK, SLOTS_AHEAD = 2, 4


def finish_kernel(left_ref, gath_ref, inv_ref, noise_ref, out_ref, z_ref, held, inv_held, sems, inv_sem):
    count = SOURCES // BLOCK
    lane = lax.broadcasted_iota(jnp.int32, (4, 8, 128), 2)

    def fetch(b):
        slot = lax.rem(b, SLOTS_AHEAD)
        return pltpu.make_async_copy(
            left_ref.at[pl.ds(b * BLOCK, BLOCK)], held.at[slot], sems.at[slot]
        )

    inverse = pltpu.make_async_copy(inv_ref, inv_held, inv_sem)
    for b in range(SLOTS_AHEAD - 1):
        fetch(b).start()
    inverse.start()
    first = gath_ref[0].astype(f32)
    where = lax.broadcasted_iota(jnp.int32, (DEPTH, 128), 0) < 2 * SLOTS
    where &= lax.broadcasted_iota(jnp.int32, (DEPTH, 128), 1) < SITES

    def some(b, squares):
        @pl.when(b + SLOTS_AHEAD - 1 < count)
        def _():
            fetch(b + SLOTS_AHEAD - 1).start()

        fetch(b).wait()
        slot = lax.rem(b, SLOTS_AHEAD)
        for i in range(BLOCK):
            f = b * BLOCK + i
            block = gath_ref[f]
            wide = block.astype(f32)
            squares = squares + wide * wide
            left = held[slot, i].reshape(CHUNKS * 8 * ROWS, 256)[:, :DEPTH]
            prod = lax.dot_general(left, block, PLAIN, preferred_element_type=f32)
            prod = prod.reshape(CHUNKS, 4, 4, 8, 128)
            packed = []
            for g in range(CHUNKS):
                acc = jnp.zeros((4, 8, 128), f32)
                for r in range(4):
                    moved = pltpu.roll(prod[g, :, r], (32 * r - SITES * g) % 128, 2)
                    acc = jnp.where((lane >= 32 * r) & (lane < 32 * r + SITES), moved, acc)
                packed.append(acc)
            start = pl.multiple_of(f * CHUNKS * 8, 16)
            for q in range(4):
                col = jnp.concatenate([packed[g][q] for g in range(CHUNKS)], axis=0)
                z_ref[pl.ds(start, CHUNKS * 8), 128 * q : 128 * (q + 1)] = col.astype(bf16)
        return squares

    squares = lax.fori_loop(0, count, some, jnp.where(where, -0.5 * first * first, 0.0))
    spots = jnp.sum(squares * noise_ref[...], axis=0, keepdims=True) * (2.0 / PERIOD)
    noise = spots
    for g in range(1, CHUNKS):
        noise = noise + pltpu.roll(spots, 128 - SITES * g, 1)
    noise = jnp.where(lax.broadcasted_iota(jnp.int32, (1, 128), 1) < SITES, noise, 0.0)
    noise = jnp.concatenate([noise, jnp.zeros((1, WIDE - 128), f32)], axis=1)
    row = lax.broadcasted_iota(jnp.int32, (32, WIDE), 0)
    tail = jnp.zeros((32, WIDE), f32)
    for n, part in enumerate(three(noise)):
        tail = jnp.where(row == SITES + n, part, tail)
    inverse.wait()
    total = lax.dot_general(inv_held[...], z_ref[...], PLAIN, preferred_element_type=f32)
    total = (total.T * (2.0 / PERIOD)).reshape(ROWS, 32, WIDE) + tail[None]
    out_ref[...] = total[:, :24].astype(bf16)


def finish(left, gathered, inverse, slot_noise):
    vmem = pl.BlockSpec(memory_space=pltpu.VMEM)
    hbm = pl.BlockSpec(memory_space=pl.ANY)
    return pl.pallas_call(
        finish_kernel,
        in_specs=[hbm, vmem, hbm, vmem],
        out_specs=vmem,
        out_shape=jax.ShapeDtypeStruct((ROWS, 24, WIDE), bf16),
        scratch_shapes=[
            pltpu.VMEM((TALL, 4 * 128), bf16),
            pltpu.VMEM((SLOTS_AHEAD, BLOCK, CHUNKS, 8 * ROWS, 256), bf16),
            pltpu.VMEM((WIDE, TALL), bf16),
            pltpu.SemaphoreType.DMA((SLOTS_AHEAD,)),
            pltpu.SemaphoreType.DMA,
        ],
        name="finish",
    )(left, gathered, inverse, slot_noise)


def total_kernel(got_ref, rep_ref, noise_ref):
    total = jnp.sum(got_ref[...].astype(f32), axis=0)
    rep_ref[...] = jnp.broadcast_to(total.astype(bf16)[None], rep_ref.shape)
    tail = total[16:24, :128]
    row = lax.broadcasted_iota(jnp.int32, tail.shape, 0)
    noise_ref[...] = jnp.sum(jnp.where(row >= SITES - 16, tail, 0.0), axis=0, keepdims=True)


def total_of(got):
    vmem = pl.BlockSpec(memory_space=pltpu.VMEM)
    return pl.pallas_call(
        total_kernel,
        in_specs=[vmem],
        out_specs=[vmem] * 2,
        out_shape=[
            jax.ShapeDtypeStruct(got.shape, bf16),
            jax.ShapeDtypeStruct((1, 128), f32),
        ],
        compiler_params=pltpu.CompilerParams(vmem_limit_bytes=8 << 20),
        name="total",
    )(got)


def share(array, axis):
    n = lax.axis_size(axis)
    return lax.all_to_all(
        jnp.broadcast_to(array[None], (n, *array.shape)), axis, 0, 0, tiled=True
    )


def payload_of(response, advance_offset, first_bin):
    k_own = first_bin + lax.iota(jnp.int32, BINS)
    turn = (k_own[:, None] * advance_offset[None, :]) % PERIOD
    ang = turn.astype(f32) * (2.0 * math.pi / PERIOD)
    cos, sin = jnp.cos(ang)[:, None, :], jnp.sin(ang)[:, None, :]
    re, im = response[:, 0].astype(f32), response[:, 1].astype(f32)
    turned = jnp.stack([re * cos - im * sin, re * sin + im * cos], axis=1).astype(bf16)
    half = turned.reshape(2 * BINS, SLOTS, SITES)
    half = jnp.pad(half, ((0, CHUNKS * HALVES - 2 * BINS), (0, 0), (0, 0)))
    half = half.reshape(CHUNKS, DEPTH, SITES).transpose(1, 0, 2).reshape(DEPTH, CHUNKS * SITES)
    return jnp.pad(half, ((0, 0), (0, 128 - CHUNKS * SITES)))


def noise_of(slot_sensor, sensor_noise):
    ids = lax.iota(jnp.int32, sensor_noise.shape[0])
    slot_noise = jnp.sum(
        jnp.where(slot_sensor[:, None] == ids[None, :], sensor_noise[None, :], 0.0), axis=1
    )
    return jnp.tile(slot_noise, HALVES)[:, None]


def on_device(samples, response, slot_sensor, sensor_noise, advance_offset):
    first_bin = lax.axis_index(FREQ) * BINS
    payload = payload_of(response, advance_offset, first_bin)
    gathered = share(share(payload, Z), X).reshape(SOURCES, DEPTH, 128)
    left, inverse = spread(samples, (slot_sensor >= 0).astype(bf16)[:, None])
    piece = finish(left, gathered, inverse, noise_of(slot_sensor, sensor_noise))
    got = lax.all_to_all(piece, SENS, 0, 0, tiled=True)
    copies, noise = total_of(got)
    outlook = lax.all_to_all(copies, SENS, 0, 0, tiled=True)[:, :SITES, :STEPS]
    return outlook, noise[0, :SITES]


def solution(mesh):
    torus = Mesh(mesh.devices.reshape(4, 8, 8, 2), (X, Z, Y, C))
    return jax.shard_map(
        on_device,
        mesh=torus,
        in_specs=(P(FREQ, SENS, None), P(FREQ, None, SENS, None), P(SENS), P(), P()),
        out_specs=(P(FREQ, None, None), P()),
        check_vma=False,
    )
```

```python
import math

import jax
import jax.numpy as jnp
import numpy as np
from jax import lax
from jax.experimental import pallas as pl
from jax.experimental.pallas import tpu as pltpu
from jax.sharding import Mesh
from jax.sharding import PartitionSpec as P

KEPT = 448
PERIOD = 2 * KEPT
BINS, SLOTS, SITES, STEPS, ROWS = 14, 40, 21, 420, 16
SOURCES = KEPT // BINS
CHUNKS, HALVES = 6, 5
DEPTH = HALVES * SLOTS
TALL = SOURCES * CHUNKS * 8
WIDE = 512
X, Z, Y, C = "freq_0", "freq_1", "sens_0", "sens_1"
FREQ = (X, Z)
SENS = (Y, C)
f32, bf16 = jnp.float32, jnp.bfloat16
PLAIN = (((1,), (0,)), ((), ()))
TURNED = (((1,), (1,)), ((), ()))


def base_table():
    k = np.arange(KEPT)[:, None]
    t = np.arange(STEPS)[None, :]
    a = ((k * t) % PERIOD) * (2.0 * np.pi / PERIOD)
    return np.stack([np.cos(a), -np.sin(a)], axis=1)


def chunk_rows():
    table = base_table().reshape(SOURCES, BINS, 2, STEPS)
    table = np.pad(table, ((0, 0), (0, 2), (0, 0), (0, WIDE - STEPS)))
    parts = [table[:, 5 * g // 2 : 5 * g // 2 + 4] for g in range(CHUNKS)]
    return np.stack(parts, axis=1).swapaxes(2, 3).reshape(TALL, WIDE)


def chunk_masks():
    same = np.zeros((CHUNKS, 2, 4, 256), np.float32)
    swap = np.zeros((CHUNKS, 2, 4, 256), np.float32)
    for g in range(CHUNKS):
        for h in range(HALVES):
            half = 5 * g + h
            if half < 2 * BINS:
                b = half // 2 - 5 * g // 2
                lanes = slice(h * SLOTS, (h + 1) * SLOTS)
                if half % 2 == 0:
                    same[g, :, b, lanes] = 1.0
                else:
                    swap[g, 0, b, lanes] = -1.0
                    swap[g, 1, b, lanes] = 1.0
    return same.reshape(CHUNKS, 8, 256), swap.reshape(CHUNKS, 8, 256)


def spread_kernel(
    pay_ref, x_ref, live_ref, noise_ref, table_ref, same_ref, swap_ref,
    rep_ref, out_ref, inv_ref, col_ref, x5_ref,
):
    rep_ref[...] = jnp.broadcast_to(pay_ref[...][None], rep_ref.shape)
    rows = table_ref[...].astype(f32)
    place = lax.broadcasted_iota(jnp.int32, (TALL, WIDE), 0)
    inv_ref[...] = (rows * jnp.where((place == 0) | (place == 4), 0.5, 1.0)).T.astype(bf16)
    x5_ref[...] = jnp.zeros_like(x5_ref)
    for h in range(HALVES):
        col_ref[h * SLOTS : (h + 1) * SLOTS] = noise_ref[...]

    def pair(p, carry):
        halves = []
        for j in range(2):
            x = x_ref[2 * p + j] * live_ref[...]
            for h in range(HALVES):
                x5_ref[j, h * SLOTS : (h + 1) * SLOTS, :STEPS] = x
            d = lax.dot_general(table_ref[...], x5_ref[j], TURNED, preferred_element_type=f32)
            d = d.reshape(SOURCES, CHUNKS, 8, 256)
            halves.append(d * same_ref[...][None] + pltpu.roll(d, 4, 2) * swap_ref[...][None])
        both = jnp.concatenate(halves, axis=2).astype(bf16)
        out_ref[:, :, pl.ds(pl.multiple_of(16 * p, 16), 16), :] = both
        return carry

    lax.fori_loop(0, ROWS // 2, pair, 0)


def spread(payload, samples, live, noise):
    same, swap = chunk_masks()
    vmem = pl.BlockSpec(memory_space=pltpu.VMEM)
    return pl.pallas_call(
        spread_kernel,
        in_specs=[vmem] * 7,
        out_specs=[vmem] * 4,
        out_shape=[
            pltpu.VMEM((8, DEPTH, 128), bf16),
            pltpu.VMEM((SOURCES, CHUNKS, 8 * ROWS, 256), bf16),
            pltpu.VMEM((WIDE, TALL), bf16),
            pltpu.VMEM((DEPTH, 1), f32),
        ],
        scratch_shapes=[pltpu.VMEM((2, 256, WIDE), bf16)],
        cost_estimate=pl.CostEstimate(
            flops=2 * TALL * WIDE * 256 * ROWS, transcendentals=0, bytes_accessed=16_000_000
        ),
        compiler_params=pltpu.CompilerParams(vmem_limit_bytes=24 << 20),
        name="spread",
    )(payload, samples, live, noise, jnp.asarray(chunk_rows(), bf16), jnp.asarray(same), jnp.asarray(swap))


def three(v):
    hi = v.astype(bf16).astype(f32)
    mid = (v - hi).astype(bf16).astype(f32)
    return hi, mid, v - hi - mid


UNROLL = 4


def finish_kernel(left_ref, gath_ref, inv_ref, noise_ref, out_ref, z_ref):
    lane = lax.broadcasted_iota(jnp.int32, (4, 8, 128), 2)
    first = gath_ref[0].astype(f32)
    where = lax.broadcasted_iota(jnp.int32, (DEPTH, 128), 0) < 2 * SLOTS
    where &= lax.broadcasted_iota(jnp.int32, (DEPTH, 128), 1) < SITES

    def some(s, squares):
        for i in range(UNROLL):
            f = s * UNROLL + i
            block = gath_ref[f]
            wide = block.astype(f32)
            squares = squares + wide * wide
            left = left_ref[f].reshape(CHUNKS * 8 * ROWS, 256)[:, :DEPTH]
            prod = lax.dot_general(left, block, PLAIN, preferred_element_type=f32)
            prod = prod.reshape(CHUNKS, 4, 4, 8, 128)
            packed = []
            for g in range(CHUNKS):
                acc = jnp.zeros((4, 8, 128), f32)
                for r in range(4):
                    moved = pltpu.roll(prod[g, :, r], (32 * r - SITES * g) % 128, 2)
                    acc = jnp.where((lane >= 32 * r) & (lane < 32 * r + SITES), moved, acc)
                packed.append(acc)
            start = pl.multiple_of(f * CHUNKS * 8, 16)
            for q in range(4):
                col = jnp.concatenate([packed[g][q] for g in range(CHUNKS)], axis=0)
                z_ref[pl.ds(start, CHUNKS * 8), 128 * q : 128 * (q + 1)] = col.astype(bf16)
        return squares

    squares = lax.fori_loop(
        0, SOURCES // UNROLL, some, jnp.where(where, -0.5 * first * first, 0.0)
    )
    spots = jnp.sum(squares * noise_ref[...], axis=0, keepdims=True) * (2.0 / PERIOD)
    noise = spots
    for g in range(1, CHUNKS):
        noise = noise + pltpu.roll(spots, 128 - SITES * g, 1)
    noise = jnp.where(lax.broadcasted_iota(jnp.int32, (1, 128), 1) < SITES, noise, 0.0)
    noise = jnp.concatenate([noise, jnp.zeros((1, WIDE - 128), f32)], axis=1)
    row = lax.broadcasted_iota(jnp.int32, (32, WIDE), 0)
    tail = jnp.zeros((32, WIDE), f32)
    for n, part in enumerate(three(noise)):
        tail = jnp.where(row == SITES + n, part, tail)
    total = lax.dot_general(inv_ref[...], z_ref[...], PLAIN, preferred_element_type=f32)
    total = (total.T * (2.0 / PERIOD)).reshape(ROWS, 32, WIDE) + tail[None]
    out_ref[...] = total[:, :24].astype(bf16)


def finish(left, gathered, inverse, slot_noise):
    vmem = pl.BlockSpec(memory_space=pltpu.VMEM)
    return pl.pallas_call(
        finish_kernel,
        in_specs=[vmem] * 4,
        out_specs=vmem,
        out_shape=pltpu.VMEM((ROWS, 24, WIDE), bf16),
        scratch_shapes=[pltpu.VMEM((TALL, 4 * 128), bf16)],
        compiler_params=pltpu.CompilerParams(vmem_limit_bytes=24 << 20),
        name="finish",
    )(left, gathered, inverse, slot_noise)


def total_kernel(got_ref, rep_ref, noise_ref):
    total = jnp.sum(got_ref[...].astype(f32), axis=0)
    rep_ref[...] = jnp.broadcast_to(total.astype(bf16)[None], rep_ref.shape)
    tail = total[16:24, :SITES]
    row = lax.broadcasted_iota(jnp.int32, tail.shape, 0)
    noise_ref[...] = jnp.sum(jnp.where(row >= SITES - 16, tail, 0.0), axis=0, keepdims=True)


def total_of(got):
    vmem = pl.BlockSpec(memory_space=pltpu.VMEM)
    return pl.pallas_call(
        total_kernel,
        in_specs=[vmem],
        out_specs=[vmem] * 2,
        out_shape=[
            pltpu.VMEM(got.shape, bf16),
            jax.ShapeDtypeStruct((1, SITES), f32),
        ],
        compiler_params=pltpu.CompilerParams(vmem_limit_bytes=8 << 20),
        name="total",
    )(got)


def share(array, axis):
    n = lax.axis_size(axis)
    return lax.all_to_all(
        jnp.broadcast_to(array[None], (n, *array.shape)), axis, 0, 0, tiled=True
    )


def payload_of(response, advance_offset, first_bin):
    k_own = first_bin + lax.iota(jnp.int32, BINS)
    turn = (k_own[:, None] * advance_offset[None, :]) % PERIOD
    ang = turn.astype(f32) * (2.0 * math.pi / PERIOD)
    cos, sin = jnp.cos(ang)[:, None, :], jnp.sin(ang)[:, None, :]
    re, im = response[:, 0].astype(f32), response[:, 1].astype(f32)
    turned = jnp.stack([re * cos - im * sin, re * sin + im * cos], axis=1).astype(bf16)
    half = turned.reshape(2 * BINS, SLOTS, SITES)
    half = jnp.pad(half, ((0, CHUNKS * HALVES - 2 * BINS), (0, 0), (0, 0)))
    half = half.reshape(CHUNKS, DEPTH, SITES).transpose(1, 0, 2).reshape(DEPTH, CHUNKS * SITES)
    return jnp.pad(half, ((0, 0), (0, 128 - CHUNKS * SITES)))


def noise_of(slot_sensor, sensor_noise):
    ids = lax.iota(jnp.int32, sensor_noise.shape[0])
    slot_noise = jnp.sum(
        jnp.where(slot_sensor[:, None] == ids[None, :], sensor_noise[None, :], 0.0), axis=1
    )
    return slot_noise[:, None]


def on_device(samples, response, slot_sensor, sensor_noise, advance_offset):
    first_bin = lax.axis_index(FREQ) * BINS
    payload = payload_of(response, advance_offset, first_bin)
    live = (slot_sensor >= 0).astype(bf16)[:, None]
    copies, left, inverse, column = spread(
        payload, samples, live, noise_of(slot_sensor, sensor_noise)
    )
    gathered = share(lax.all_to_all(copies, Z, 0, 0, tiled=True), X)
    gathered = gathered.reshape(SOURCES, DEPTH, 128)
    piece = finish(left, gathered, inverse, column)
    got = lax.all_to_all(piece, SENS, 0, 0, tiled=True)
    copies, noise = total_of(got)
    copies, noise = lax.optimization_barrier((copies, noise.reshape(SITES)))
    outlook = lax.all_to_all(copies, SENS, 0, 0, tiled=True)[:, :SITES, :STEPS]
    return outlook, noise


def solution(mesh):
    torus = Mesh(mesh.devices.reshape(4, 8, 8, 2), (X, Z, Y, C))
    return jax.shard_map(
        on_device,
        mesh=torus,
        in_specs=(P(FREQ, SENS, None), P(FREQ, None, SENS, None), P(SENS), P(), P()),
        out_specs=(P(FREQ, None, None), P()),
        check_vma=False,
    )
```

```python
import math

import jax
import jax.numpy as jnp
import numpy as np
from jax import lax
from jax.experimental import pallas as pl
from jax.experimental.pallas import tpu as pltpu
from jax.sharding import Mesh
from jax.sharding import PartitionSpec as P

KEPT = 448
PERIOD = 2 * KEPT
BINS, SLOTS, SITES, STEPS, ROWS = 14, 40, 21, 420, 16
SOURCES = KEPT // BINS
CHUNKS, HALVES = 6, 5
DEPTH = HALVES * SLOTS
TALL = SOURCES * CHUNKS * 8
WIDE = 512
X, Z, Y, C = "freq_0", "freq_1", "sens_0", "sens_1"
FREQ = (X, Z)
SENS = (Y, C)
f32, bf16 = jnp.float32, jnp.bfloat16
PLAIN = (((1,), (0,)), ((), ()))
TURNED = (((1,), (1,)), ((), ()))


def base_table():
    k = np.arange(KEPT)[:, None]
    t = np.arange(STEPS)[None, :]
    a = ((k * t) % PERIOD) * (2.0 * np.pi / PERIOD)
    return np.stack([np.cos(a), -np.sin(a)], axis=1)


def chunk_rows():
    table = base_table().reshape(SOURCES, BINS, 2, STEPS)
    table = np.pad(table, ((0, 0), (0, 2), (0, 0), (0, WIDE - STEPS)))
    parts = [table[:, 5 * g // 2 : 5 * g // 2 + 4] for g in range(CHUNKS)]
    return np.stack(parts, axis=1).swapaxes(2, 3).reshape(TALL, WIDE)


def chunk_masks():
    same = np.zeros((CHUNKS, 2, 4, 256), np.float32)
    swap = np.zeros((CHUNKS, 2, 4, 256), np.float32)
    for g in range(CHUNKS):
        for h in range(HALVES):
            half = 5 * g + h
            if half < 2 * BINS:
                b = half // 2 - 5 * g // 2
                lanes = slice(h * SLOTS, (h + 1) * SLOTS)
                if half % 2 == 0:
                    same[g, :, b, lanes] = 1.0
                else:
                    swap[g, 0, b, lanes] = -1.0
                    swap[g, 1, b, lanes] = 1.0
    return same.reshape(CHUNKS, 8, 256), swap.reshape(CHUNKS, 8, 256)


def spread_kernel(
    x_ref, live_ref, noise_ref, table_ref, same_ref, swap_ref, out_ref, inv_ref, col_ref, x5_ref
):
    rows = table_ref[...].astype(f32)
    place = lax.broadcasted_iota(jnp.int32, (TALL, WIDE), 0)
    inv_ref[...] = (rows * jnp.where((place == 0) | (place == 4), 0.5, 1.0)).T.astype(bf16)
    x5_ref[...] = jnp.zeros_like(x5_ref)
    for h in range(HALVES):
        col_ref[h * SLOTS : (h + 1) * SLOTS] = noise_ref[...]

    def pair(p, carry):
        halves = []
        for j in range(2):
            x = x_ref[2 * p + j] * live_ref[...]
            for h in range(HALVES):
                x5_ref[j, h * SLOTS : (h + 1) * SLOTS, :STEPS] = x
            d = lax.dot_general(table_ref[...], x5_ref[j], TURNED, preferred_element_type=f32)
            d = d.reshape(SOURCES, CHUNKS, 8, 256)
            halves.append(d * same_ref[...][None] + pltpu.roll(d, 4, 2) * swap_ref[...][None])
        both = jnp.concatenate(halves, axis=2).astype(bf16)
        out_ref[:, :, pl.ds(pl.multiple_of(16 * p, 16), 16), :] = both
        return carry

    lax.fori_loop(0, ROWS // 2, pair, 0)


def spread(samples, live, noise):
    same, swap = chunk_masks()
    vmem = pl.BlockSpec(memory_space=pltpu.VMEM)
    return pl.pallas_call(
        spread_kernel,
        in_specs=[vmem] * 6,
        out_specs=[vmem] * 3,
        out_shape=[
            pltpu.VMEM((SOURCES, CHUNKS, 8 * ROWS, 256), bf16),
            pltpu.VMEM((WIDE, TALL), bf16),
            pltpu.VMEM((DEPTH, 1), f32),
        ],
        scratch_shapes=[pltpu.VMEM((2, 256, WIDE), bf16)],
        cost_estimate=pl.CostEstimate(
            flops=2 * TALL * WIDE * 256 * ROWS, transcendentals=0, bytes_accessed=16_000_000
        ),
        compiler_params=pltpu.CompilerParams(vmem_limit_bytes=24 << 20),
        name="spread",
    )(samples, live, noise, jnp.asarray(chunk_rows(), bf16), jnp.asarray(same), jnp.asarray(swap))


def three(v):
    hi = v.astype(bf16).astype(f32)
    mid = (v - hi).astype(bf16).astype(f32)
    return hi, mid, v - hi - mid


UNROLL = 4


def contract(f, block, left_ref, lane):
    left = left_ref[f].reshape(CHUNKS * 8 * ROWS, 256)[:, :DEPTH]
    prod = lax.dot_general(left, block, PLAIN, preferred_element_type=f32)
    prod = prod.reshape(CHUNKS, 4, 4, 8, 128)
    packed = []
    for g in range(CHUNKS):
        acc = jnp.zeros((4, 8, 128), f32)
        for r in range(4):
            moved = pltpu.roll(prod[g, :, r], (32 * r - SITES * g) % 128, 2)
            acc = jnp.where((lane >= 32 * r) & (lane < 32 * r + SITES), moved, acc)
        packed.append(acc)
    cols = [jnp.concatenate([packed[g][q] for g in range(CHUNKS)], axis=0) for q in range(4)]
    return jnp.concatenate(cols, axis=1).astype(bf16)


def walk(ref, base, row0, count, left_ref, z_ref, lane, where, squares):
    def some(s, squares):
        for i in range(UNROLL):
            n = s * UNROLL + i
            f = base + n
            block = ref[n]
            wide = block.astype(f32)
            wide = wide * wide
            squares = squares + jnp.where(where & (f == 0), 0.5 * wide, wide)
            start = pl.multiple_of((row0 + n) * CHUNKS * 8, 16)
            z_ref[pl.ds(start, CHUNKS * 8), :] = contract(f, block, left_ref, lane)
        return squares

    return lax.fori_loop(0, count // UNROLL, some, squares)


def corner():
    where = lax.broadcasted_iota(jnp.int32, (DEPTH, 128), 0) < 2 * SLOTS
    return where & (lax.broadcasted_iota(jnp.int32, (DEPTH, 128), 1) < SITES)


def near_kernel(x_ref, left_ref, own_ref, prev_ref, next_ref, inv_ref, total_ref, sq_ref, z_ref):
    lane = lax.broadcasted_iota(jnp.int32, (4, 8, 128), 2)
    where = corner()
    squares = jnp.zeros((DEPTH, 128), f32)
    x = x_ref[0]
    for ref, off in ((own_ref, 0), (prev_ref, 3), (next_ref, 1)):
        base = lax.rem(x + off, 4) * 8
        squares = walk(ref, base, base, 8, left_ref, z_ref, lane, where, squares)
    far = pl.multiple_of(lax.rem(x + 2, 4) * FAR, 16)
    z_ref[pl.ds(far, FAR), :] = jnp.zeros((FAR, WIDE), bf16)
    sq_ref[...] = squares
    total_ref[...] = lax.dot_general(inv_ref[...], z_ref[...], PLAIN, preferred_element_type=f32)


FAR = 8 * CHUNKS * 8


def near(x, left, own, prev, after, inverse):
    vmem = pl.BlockSpec(memory_space=pltpu.VMEM)
    return pl.pallas_call(
        near_kernel,
        in_specs=[pl.BlockSpec(memory_space=pltpu.SMEM)] + [vmem] * 5,
        out_specs=[vmem] * 2,
        out_shape=[pltpu.VMEM((WIDE, WIDE), f32), pltpu.VMEM((DEPTH, 128), f32)],
        scratch_shapes=[pltpu.VMEM((TALL, WIDE), bf16)],
        compiler_params=pltpu.CompilerParams(vmem_limit_bytes=20 << 20),
        cost_estimate=pl.CostEstimate(
            flops=2 * 24 * 768 * 256 * 128 + 2 * TALL * WIDE * WIDE,
            transcendentals=0,
            bytes_accessed=14_000_000,
        ),
        name="finish_near",
    )(x, left, own, prev, after, inverse)


def far_kernel(x_ref, left_ref, one_ref, two_ref, inv_ref, total_ref, sq_ref, noise_ref, out_ref, z_ref):
    lane = lax.broadcasted_iota(jnp.int32, (4, 8, 128), 2)
    where = corner()
    squares = sq_ref[...]
    far = lax.rem(x_ref[0] + 2, 4)
    for h, ref in enumerate((one_ref, two_ref)):
        squares = walk(ref, far * 8 + 4 * h, 4 * h, 4, left_ref, z_ref, lane, where, squares)
    spots = jnp.sum(squares * noise_ref[...], axis=0, keepdims=True) * (2.0 / PERIOD)
    noise = spots
    for g in range(1, CHUNKS):
        noise = noise + pltpu.roll(spots, 128 - SITES * g, 1)
    noise = jnp.where(lax.broadcasted_iota(jnp.int32, (1, 128), 1) < SITES, noise, 0.0)
    noise = jnp.concatenate([noise, jnp.zeros((1, WIDE - 128), f32)], axis=1)
    row = lax.broadcasted_iota(jnp.int32, (32, WIDE), 0)
    tail = jnp.zeros((32, WIDE), f32)
    for n, part in enumerate(three(noise)):
        tail = jnp.where(row == SITES + n, part, tail)
    inv = inv_ref[:, pl.ds(pl.multiple_of(far * FAR, 128), FAR)]
    total = total_ref[...] + lax.dot_general(inv, z_ref[...], PLAIN, preferred_element_type=f32)
    total = (total.T * (2.0 / PERIOD)).reshape(ROWS, 32, WIDE) + tail[None]
    out_ref[...] = total[:, :24].astype(bf16)


def finish_far(x, left, one, two, inverse, total, squares, column):
    vmem = pl.BlockSpec(memory_space=pltpu.VMEM)
    return pl.pallas_call(
        far_kernel,
        in_specs=[pl.BlockSpec(memory_space=pltpu.SMEM)] + [vmem] * 7,
        out_specs=vmem,
        out_shape=pltpu.VMEM((ROWS, 24, WIDE), bf16),
        scratch_shapes=[pltpu.VMEM((FAR, WIDE), bf16)],
        compiler_params=pltpu.CompilerParams(vmem_limit_bytes=20 << 20),
        name="finish_far",
    )(x, left, one, two, inverse, total, squares, column)


def step_by(array, shift):
    n = lax.axis_size(X)
    return lax.ppermute(array, X, [(i, (i + shift) % n) for i in range(n)])


def total_kernel(got_ref, rep_ref, noise_ref):
    total = jnp.sum(got_ref[...].astype(f32), axis=0)
    rep_ref[...] = jnp.broadcast_to(total.astype(bf16)[None], rep_ref.shape)
    tail = total[16:24, :SITES]
    row = lax.broadcasted_iota(jnp.int32, tail.shape, 0)
    noise_ref[...] = jnp.sum(jnp.where(row >= SITES - 16, tail, 0.0), axis=0, keepdims=True)


def total_of(got):
    vmem = pl.BlockSpec(memory_space=pltpu.VMEM)
    return pl.pallas_call(
        total_kernel,
        in_specs=[vmem],
        out_specs=[vmem] * 2,
        out_shape=[
            pltpu.VMEM(got.shape, bf16),
            jax.ShapeDtypeStruct((1, SITES), f32),
        ],
        compiler_params=pltpu.CompilerParams(vmem_limit_bytes=8 << 20),
        name="total",
    )(got)


def share(array, axis):
    n = lax.axis_size(axis)
    return lax.all_to_all(
        jnp.broadcast_to(array[None], (n, *array.shape)), axis, 0, 0, tiled=True
    )


def payload_of(response, advance_offset, first_bin):
    k_own = first_bin + lax.iota(jnp.int32, BINS)
    turn = (k_own[:, None] * advance_offset[None, :]) % PERIOD
    ang = turn.astype(f32) * (2.0 * math.pi / PERIOD)
    cos, sin = jnp.cos(ang)[:, None, :], jnp.sin(ang)[:, None, :]
    re, im = response[:, 0].astype(f32), response[:, 1].astype(f32)
    turned = jnp.stack([re * cos - im * sin, re * sin + im * cos], axis=1).astype(bf16)
    half = turned.reshape(2 * BINS, SLOTS, SITES)
    half = jnp.pad(half, ((0, CHUNKS * HALVES - 2 * BINS), (0, 0), (0, 0)))
    half = half.reshape(CHUNKS, DEPTH, SITES).transpose(1, 0, 2).reshape(DEPTH, CHUNKS * SITES)
    return jnp.pad(half, ((0, 0), (0, 128 - CHUNKS * SITES)))


def noise_of(slot_sensor, sensor_noise):
    ids = lax.iota(jnp.int32, sensor_noise.shape[0])
    slot_noise = jnp.sum(
        jnp.where(slot_sensor[:, None] == ids[None, :], sensor_noise[None, :], 0.0), axis=1
    )
    return slot_noise[:, None]


def on_device(samples, response, slot_sensor, sensor_noise, advance_offset):
    first_bin = lax.axis_index(FREQ) * BINS
    payload = payload_of(response, advance_offset, first_bin)
    own, slot_sensor, sensor_noise = lax.optimization_barrier(
        (share(payload, Z), slot_sensor, sensor_noise)
    )
    live = (slot_sensor >= 0).astype(bf16)[:, None]
    left, inverse, column = spread(samples, live, noise_of(slot_sensor, sensor_noise))
    prev, after = step_by(own, 1), step_by(own, -1)
    prev, after, left, inverse, column = lax.optimization_barrier(
        (prev, after, left, inverse, column)
    )
    x = lax.axis_index(X).astype(jnp.int32).reshape(1)
    total, squares = near(x, left, own, prev, after, inverse)
    one, two = step_by(prev[:4], 1), step_by(after[4:], -1)
    piece = finish_far(x, left, one, two, inverse, total, squares, column)
    got = lax.all_to_all(piece, SENS, 0, 0, tiled=True)
    copies, noise = total_of(got)
    copies, noise = lax.optimization_barrier((copies, noise.reshape(SITES)))
    outlook = lax.all_to_all(copies, SENS, 0, 0, tiled=True)[:, :SITES, :STEPS]
    return outlook, noise


def solution(mesh):
    torus = Mesh(mesh.devices.reshape(4, 8, 8, 2), (X, Z, Y, C))
    return jax.shard_map(
        on_device,
        mesh=torus,
        in_specs=(P(FREQ, SENS, None), P(FREQ, None, SENS, None), P(SENS), P(), P()),
        out_specs=(P(FREQ, None, None), P()),
        check_vma=False,
    )
```

```python
import math

import jax
import jax.numpy as jnp
import numpy as np
from jax import lax
from jax.experimental import pallas as pl
from jax.experimental.pallas import tpu as pltpu
from jax.sharding import Mesh
from jax.sharding import PartitionSpec as P

KEPT = 448
PERIOD = 2 * KEPT
BINS, SLOTS, SITES, STEPS, ROWS = 14, 40, 21, 420, 16
SOURCES = KEPT // BINS
CHUNKS, HALVES = 6, 5
DEPTH = HALVES * SLOTS
TALL = SOURCES * CHUNKS * 8
WIDE = 512
X, Z, Y, C = "freq_0", "freq_1", "sens_0", "sens_1"
FREQ = (X, Z)
SENS = (Y, C)
f32, bf16 = jnp.float32, jnp.bfloat16
PLAIN = (((1,), (0,)), ((), ()))
TURNED = (((1,), (1,)), ((), ()))


def base_table():
    k = np.arange(KEPT)[:, None]
    t = np.arange(STEPS)[None, :]
    a = ((k * t) % PERIOD) * (2.0 * np.pi / PERIOD)
    return np.stack([np.cos(a), -np.sin(a)], axis=1)


def chunk_rows():
    table = base_table().reshape(SOURCES, BINS, 2, STEPS)
    table = np.pad(table, ((0, 0), (0, 2), (0, 0), (0, WIDE - STEPS)))
    parts = [table[:, 5 * g // 2 : 5 * g // 2 + 4] for g in range(CHUNKS)]
    return np.stack(parts, axis=1).swapaxes(2, 3).reshape(TALL, WIDE)


def chunk_mask():
    mask = np.zeros((CHUNKS, 2, 4, 256), np.float32)
    for g in range(CHUNKS):
        for h in range(HALVES):
            half = 5 * g + h
            if half < 2 * BINS:
                mask[g, :, half // 2 - 5 * g // 2, h * SLOTS : (h + 1) * SLOTS] = 1.0
    return mask.reshape(CHUNKS, 8, 256)


def places():
    put = np.zeros((3, 256, 256), np.float32)
    for n in range(3):
        for h in range(HALVES):
            for s in range(SLOTS):
                put[n, 128 * (h % 2) + n * SLOTS + s, h * SLOTS + s] = 1.0
    return put


TRIPLES = -(-ROWS // 3)


def spread_kernel(
    x_ref, live_ref, noise_ref, table_ref, mask_ref, put_ref,
    out_ref, inv_ref, col_ref, xs_ref, both_ref,
):
    xs_ref[...] = jnp.zeros_like(xs_ref)
    for r in range(ROWS):
        at = 128 * (r // 3) + SLOTS * (r % 3)
        xs_ref[at : at + SLOTS, :STEPS] = x_ref[r] * live_ref[...]
    rows = table_ref[...].astype(f32)
    place = lax.broadcasted_iota(jnp.int32, (TALL, WIDE), 0)
    inv_ref[...] = (rows * jnp.where((place == 0) | (place == 4), 0.5, 1.0)).T.astype(bf16)
    for h in range(HALVES):
        col_ref[h * SLOTS : (h + 1) * SLOTS] = noise_ref[...]
    shape = (SOURCES, CHUNKS, 8, 256)
    sign = jnp.where(lax.broadcasted_iota(jnp.int32, shape, 2) < 4, -1.0, 1.0)
    odd = lax.broadcasted_iota(jnp.int32, shape, 1) % 2 == 1

    def transform(t, carry):
        some = xs_ref[pl.ds(pl.multiple_of(256 * t, 256), 256), :]
        d = lax.dot_general(table_ref[...], some, TURNED, preferred_element_type=f32)
        d = d.reshape(shape)
        turned = pltpu.roll(d, 4, 2) * sign
        plain = jnp.where(odd, turned, d).reshape(TALL, 256).astype(bf16)
        turned = jnp.where(odd, d, turned).reshape(TALL, 256).astype(bf16)
        for u in range(2):
            both_ref[2 * t + u, :, :128] = plain[:, 128 * u : 128 * (u + 1)]
            both_ref[2 * t + u, :, 128:] = turned[:, 128 * u : 128 * (u + 1)]
        return carry

    lax.fori_loop(0, TRIPLES // 2, transform, 0)

    def pair(p, carry):
        halves = []
        for j in range(2):
            r = 2 * p + j
            d = lax.dot_general(
                both_ref[r // 3], put_ref[lax.rem(r, 3)], PLAIN, preferred_element_type=f32
            )
            halves.append(d.reshape(shape) * mask_ref[...][None])
        wide = jnp.concatenate(halves, axis=2).astype(bf16)
        out_ref[:, :, pl.ds(pl.multiple_of(16 * p, 16), 16), :] = wide
        return carry

    lax.fori_loop(0, ROWS // 2, pair, 0)


def spread(samples, live, noise):
    vmem = pl.BlockSpec(memory_space=pltpu.VMEM)
    return pl.pallas_call(
        spread_kernel,
        in_specs=[vmem] * 6,
        out_specs=[vmem] * 3,
        out_shape=[
            pltpu.VMEM((SOURCES, CHUNKS, 8 * ROWS, 256), bf16),
            pltpu.VMEM((WIDE, TALL), bf16),
            pltpu.VMEM((DEPTH, 1), f32),
        ],
        scratch_shapes=[
            pltpu.VMEM((TRIPLES * 128, WIDE), bf16),
            pltpu.VMEM((TRIPLES, TALL, 256), bf16),
        ],
        cost_estimate=pl.CostEstimate(
            flops=2 * TALL * WIDE * 256 * ROWS, transcendentals=0, bytes_accessed=16_000_000
        ),
        compiler_params=pltpu.CompilerParams(vmem_limit_bytes=24 << 20),
        name="spread",
    )(
        samples,
        live,
        noise,
        jnp.asarray(chunk_rows(), bf16),
        jnp.asarray(chunk_mask()),
        jnp.asarray(places(), bf16),
    )


def three(v):
    hi = v.astype(bf16).astype(f32)
    mid = (v - hi).astype(bf16).astype(f32)
    return hi, mid, v - hi - mid


UNROLL = 4


def contract(f, block, left_ref, lane):
    left = left_ref[f].reshape(CHUNKS * 8 * ROWS, 256)[:, :DEPTH]
    prod = lax.dot_general(left, block, PLAIN, preferred_element_type=f32)
    prod = prod.reshape(CHUNKS, 4, 4, 8, 128)
    packed = []
    for g in range(CHUNKS):
        acc = jnp.zeros((4, 8, 128), f32)
        for r in range(4):
            moved = pltpu.roll(prod[g, :, r], (32 * r - SITES * g) % 128, 2)
            acc = jnp.where((lane >= 32 * r) & (lane < 32 * r + SITES), moved, acc)
        packed.append(acc)
    cols = [jnp.concatenate([packed[g][q] for g in range(CHUNKS)], axis=0) for q in range(4)]
    return jnp.concatenate(cols, axis=1).astype(bf16)


def walk(ref, base, row0, count, left_ref, z_ref, lane, where, squares):
    def some(s, squares):
        for i in range(UNROLL):
            n = s * UNROLL + i
            f = base + n
            block = ref[n]
            wide = block.astype(f32)
            wide = wide * wide
            squares = squares + jnp.where(where & (f == 0), 0.5 * wide, wide)
            start = pl.multiple_of((row0 + n) * CHUNKS * 8, 16)
            z_ref[pl.ds(start, CHUNKS * 8), :] = contract(f, block, left_ref, lane)
        return squares

    return lax.fori_loop(0, count // UNROLL, some, squares)


def corner():
    where = lax.broadcasted_iota(jnp.int32, (DEPTH, 128), 0) < 2 * SLOTS
    return where & (lax.broadcasted_iota(jnp.int32, (DEPTH, 128), 1) < SITES)


def near_kernel(x_ref, left_ref, own_ref, prev_ref, next_ref, inv_ref, total_ref, sq_ref, z_ref):
    lane = lax.broadcasted_iota(jnp.int32, (4, 8, 128), 2)
    where = corner()
    squares = jnp.zeros((DEPTH, 128), f32)
    x = x_ref[0]
    for ref, off in ((own_ref, 0), (prev_ref, 3), (next_ref, 1)):
        base = lax.rem(x + off, 4) * 8
        squares = walk(ref, base, base, 8, left_ref, z_ref, lane, where, squares)
    far = pl.multiple_of(lax.rem(x + 2, 4) * FAR, 16)
    z_ref[pl.ds(far, FAR), :] = jnp.zeros((FAR, WIDE), bf16)
    sq_ref[...] = squares
    total_ref[...] = lax.dot_general(inv_ref[...], z_ref[...], PLAIN, preferred_element_type=f32)


FAR = 8 * CHUNKS * 8


def near(x, left, own, prev, after, inverse):
    vmem = pl.BlockSpec(memory_space=pltpu.VMEM)
    return pl.pallas_call(
        near_kernel,
        in_specs=[pl.BlockSpec(memory_space=pltpu.SMEM)] + [vmem] * 5,
        out_specs=[vmem] * 2,
        out_shape=[pltpu.VMEM((WIDE, WIDE), f32), pltpu.VMEM((DEPTH, 128), f32)],
        scratch_shapes=[pltpu.VMEM((TALL, WIDE), bf16)],
        compiler_params=pltpu.CompilerParams(vmem_limit_bytes=20 << 20),
        cost_estimate=pl.CostEstimate(
            flops=2 * 24 * 768 * 256 * 128 + 2 * TALL * WIDE * WIDE,
            transcendentals=0,
            bytes_accessed=14_000_000,
        ),
        name="finish_near",
    )(x, left, own, prev, after, inverse)


def far_kernel(x_ref, left_ref, one_ref, two_ref, inv_ref, total_ref, sq_ref, noise_ref, out_ref, z_ref):
    lane = lax.broadcasted_iota(jnp.int32, (4, 8, 128), 2)
    where = corner()
    squares = sq_ref[...]
    far = lax.rem(x_ref[0] + 2, 4)
    for h, ref in enumerate((one_ref, two_ref)):
        squares = walk(ref, far * 8 + 4 * h, 4 * h, 4, left_ref, z_ref, lane, where, squares)
    spots = jnp.sum(squares * noise_ref[...], axis=0, keepdims=True) * (2.0 / PERIOD)
    noise = spots
    for g in range(1, CHUNKS):
        noise = noise + pltpu.roll(spots, 128 - SITES * g, 1)
    noise = jnp.where(lax.broadcasted_iota(jnp.int32, (1, 128), 1) < SITES, noise, 0.0)
    noise = jnp.concatenate([noise, jnp.zeros((1, WIDE - 128), f32)], axis=1)
    row = lax.broadcasted_iota(jnp.int32, (32, WIDE), 0)
    tail = jnp.zeros((32, WIDE), f32)
    for n, part in enumerate(three(noise)):
        tail = jnp.where(row == SITES + n, part, tail)
    inv = inv_ref[:, pl.ds(pl.multiple_of(far * FAR, 128), FAR)]
    total = total_ref[...] + lax.dot_general(inv, z_ref[...], PLAIN, preferred_element_type=f32)
    total = (total.T * (2.0 / PERIOD)).reshape(ROWS, 32, WIDE) + tail[None]
    out_ref[...] = total[:, :24].astype(bf16)


def finish_far(x, left, one, two, inverse, total, squares, column):
    vmem = pl.BlockSpec(memory_space=pltpu.VMEM)
    return pl.pallas_call(
        far_kernel,
        in_specs=[pl.BlockSpec(memory_space=pltpu.SMEM)] + [vmem] * 7,
        out_specs=vmem,
        out_shape=pltpu.VMEM((ROWS, 24, WIDE), bf16),
        scratch_shapes=[pltpu.VMEM((FAR, WIDE), bf16)],
        compiler_params=pltpu.CompilerParams(vmem_limit_bytes=20 << 20),
        name="finish_far",
    )(x, left, one, two, inverse, total, squares, column)


def step_by(array, shift):
    n = lax.axis_size(X)
    return lax.ppermute(array, X, [(i, (i + shift) % n) for i in range(n)])


def total_kernel(got_ref, rep_ref, noise_ref):
    total = jnp.sum(got_ref[...].astype(f32), axis=0)
    rep_ref[...] = jnp.broadcast_to(total.astype(bf16)[None], rep_ref.shape)
    tail = total[16:24, :SITES]
    row = lax.broadcasted_iota(jnp.int32, tail.shape, 0)
    noise_ref[...] = jnp.sum(jnp.where(row >= SITES - 16, tail, 0.0), axis=0, keepdims=True)


def total_of(got):
    vmem = pl.BlockSpec(memory_space=pltpu.VMEM)
    return pl.pallas_call(
        total_kernel,
        in_specs=[vmem],
        out_specs=[vmem] * 2,
        out_shape=[
            pltpu.VMEM(got.shape, bf16),
            jax.ShapeDtypeStruct((1, SITES), f32),
        ],
        compiler_params=pltpu.CompilerParams(vmem_limit_bytes=8 << 20),
        name="total",
    )(got)


def share(array, axis):
    n = lax.axis_size(axis)
    return lax.all_to_all(
        jnp.broadcast_to(array[None], (n, *array.shape)), axis, 0, 0, tiled=True
    )


def payload_of(response, advance_offset, first_bin):
    k_own = first_bin + lax.iota(jnp.int32, BINS)
    turn = (k_own[:, None] * advance_offset[None, :]) % PERIOD
    ang = turn.astype(f32) * (2.0 * math.pi / PERIOD)
    cos, sin = jnp.cos(ang)[:, None, :], jnp.sin(ang)[:, None, :]
    re, im = response[:, 0].astype(f32), response[:, 1].astype(f32)
    turned = jnp.stack([re * cos - im * sin, re * sin + im * cos], axis=1).astype(bf16)
    half = turned.reshape(2 * BINS, SLOTS, SITES)
    half = jnp.pad(half, ((0, CHUNKS * HALVES - 2 * BINS), (0, 0), (0, 0)))
    half = half.reshape(CHUNKS, DEPTH, SITES).transpose(1, 0, 2).reshape(DEPTH, CHUNKS * SITES)
    return jnp.pad(half, ((0, 0), (0, 128 - CHUNKS * SITES)))


def noise_of(slot_sensor, sensor_noise):
    ids = lax.iota(jnp.int32, sensor_noise.shape[0])
    slot_noise = jnp.sum(
        jnp.where(slot_sensor[:, None] == ids[None, :], sensor_noise[None, :], 0.0), axis=1
    )
    return slot_noise[:, None]


def on_device(samples, response, slot_sensor, sensor_noise, advance_offset):
    first_bin = lax.axis_index(FREQ) * BINS
    payload = payload_of(response, advance_offset, first_bin)
    own, slot_sensor, sensor_noise = lax.optimization_barrier(
        (share(payload, Z), slot_sensor, sensor_noise)
    )
    live = (slot_sensor >= 0).astype(bf16)[:, None]
    left, inverse, column = spread(samples, live, noise_of(slot_sensor, sensor_noise))
    prev, after = step_by(own, 1), step_by(own, -1)
    prev, after, left, inverse, column = lax.optimization_barrier(
        (prev, after, left, inverse, column)
    )
    x = lax.axis_index(X).astype(jnp.int32).reshape(1)
    total, squares = near(x, left, own, prev, after, inverse)
    one, two = step_by(prev[:4], 1), step_by(after[4:], -1)
    piece = finish_far(x, left, one, two, inverse, total, squares, column)
    got = lax.all_to_all(piece, SENS, 0, 0, tiled=True)
    copies, noise = total_of(got)
    copies, noise = lax.optimization_barrier((copies, noise.reshape(SITES)))
    outlook = lax.all_to_all(copies, SENS, 0, 0, tiled=True)[:, :SITES, :STEPS]
    return outlook, noise


def solution(mesh):
    torus = Mesh(mesh.devices.reshape(4, 8, 8, 2), (X, Z, Y, C))
    return jax.shard_map(
        on_device,
        mesh=torus,
        in_specs=(P(FREQ, SENS, None), P(FREQ, None, SENS, None), P(SENS), P(), P()),
        out_specs=(P(FREQ, None, None), P()),
        check_vma=False,
    )
```

```python
import math

import jax
import jax.numpy as jnp
import numpy as np
from jax import lax
from jax.experimental import pallas as pl
from jax.experimental.pallas import tpu as pltpu
from jax.sharding import Mesh
from jax.sharding import PartitionSpec as P

KEPT = 448
PERIOD = 2 * KEPT
BINS, SLOTS, SITES, STEPS, ROWS = 14, 40, 21, 420, 16
SOURCES = KEPT // BINS
CHUNKS, HALVES = 6, 5
DEPTH = HALVES * SLOTS
TALL = SOURCES * CHUNKS * 8
WIDE = 512
X, Z, Y, C = "freq_0", "freq_1", "sens_0", "sens_1"
FREQ = (X, Z)
SENS = (Y, C)
f32, bf16 = jnp.float32, jnp.bfloat16
PLAIN = (((1,), (0,)), ((), ()))
TURNED = (((1,), (1,)), ((), ()))


def base_table():
    k = np.arange(KEPT)[:, None]
    t = np.arange(STEPS)[None, :]
    a = ((k * t) % PERIOD) * (2.0 * np.pi / PERIOD)
    return np.stack([np.cos(a), -np.sin(a)], axis=1)


def chunk_rows():
    table = base_table().reshape(SOURCES, BINS, 2, STEPS)
    table = np.pad(table, ((0, 0), (0, 2), (0, 0), (0, WIDE - STEPS)))
    parts = [table[:, 5 * g // 2 : 5 * g // 2 + 4] for g in range(CHUNKS)]
    return np.stack(parts, axis=1).swapaxes(2, 3).reshape(TALL, WIDE)


def chunk_mask():
    mask = np.zeros((CHUNKS, 2, 4, 256), np.float32)
    for g in range(CHUNKS):
        for h in range(HALVES):
            half = 5 * g + h
            if half < 2 * BINS:
                mask[g, :, half // 2 - 5 * g // 2, h * SLOTS : (h + 1) * SLOTS] = 1.0
    return mask.reshape(CHUNKS, 8, 256)


def places():
    put = np.zeros((3, 256, 256), np.float32)
    for n in range(3):
        for h in range(HALVES):
            for s in range(SLOTS):
                put[n, 128 * (h % 2) + n * SLOTS + s, h * SLOTS + s] = 1.0
    return put


TRIPLES = -(-ROWS // 3)


def spread_kernel(
    x_ref, live_ref, noise_ref, table_ref, mask_ref, put_ref,
    out_ref, inv_ref, col_ref, xs_ref, both_ref,
):
    xs_ref[...] = jnp.zeros_like(xs_ref)
    for r in range(ROWS):
        at = 128 * (r // 3) + SLOTS * (r % 3)
        xs_ref[at : at + SLOTS, :STEPS] = x_ref[r] * live_ref[...]
    rows = table_ref[...].astype(f32)
    place = lax.broadcasted_iota(jnp.int32, (TALL, WIDE), 0)
    inv_ref[...] = (rows * jnp.where((place == 0) | (place == 4), 0.5, 1.0)).T.astype(bf16)
    for h in range(HALVES):
        col_ref[h * SLOTS : (h + 1) * SLOTS] = noise_ref[...]
    shape = (SOURCES, CHUNKS, 8, 256)
    sign = jnp.where(lax.broadcasted_iota(jnp.int32, shape, 2) < 4, -1.0, 1.0)
    odd = lax.broadcasted_iota(jnp.int32, shape, 1) % 2 == 1

    def transform(t, carry):
        some = xs_ref[pl.ds(pl.multiple_of(256 * t, 256), 256), :]
        d = lax.dot_general(table_ref[...], some, TURNED, preferred_element_type=f32)
        d = d.reshape(shape)
        turned = pltpu.roll(d, 4, 2) * sign
        plain = jnp.where(odd, turned, d).reshape(TALL, 256).astype(bf16)
        turned = jnp.where(odd, d, turned).reshape(TALL, 256).astype(bf16)
        for u in range(2):
            both_ref[2 * t + u, :, :128] = plain[:, 128 * u : 128 * (u + 1)]
            both_ref[2 * t + u, :, 128:] = turned[:, 128 * u : 128 * (u + 1)]
        return carry

    lax.fori_loop(0, TRIPLES // 2, transform, 0)

    def pair(p, carry):
        halves = []
        for j in range(2):
            r = 2 * p + j
            d = lax.dot_general(
                both_ref[r // 3], put_ref[lax.rem(r, 3)], PLAIN, preferred_element_type=f32
            )
            halves.append(d.reshape(shape) * mask_ref[...][None])
        wide = jnp.concatenate(halves, axis=2).astype(bf16)
        out_ref[:, :, pl.ds(pl.multiple_of(16 * p, 16), 16), :] = wide
        return carry

    lax.fori_loop(0, ROWS // 2, pair, 0)


def spread(samples, live, noise):
    vmem = pl.BlockSpec(memory_space=pltpu.VMEM)
    return pl.pallas_call(
        spread_kernel,
        in_specs=[vmem] * 6,
        out_specs=[vmem] * 3,
        out_shape=[
            pltpu.VMEM((SOURCES, CHUNKS, 8 * ROWS, 256), bf16),
            pltpu.VMEM((WIDE, TALL), bf16),
            pltpu.VMEM((DEPTH, 1), f32),
        ],
        scratch_shapes=[
            pltpu.VMEM((TRIPLES * 128, WIDE), bf16),
            pltpu.VMEM((TRIPLES, TALL, 256), bf16),
        ],
        cost_estimate=pl.CostEstimate(
            flops=2 * TALL * WIDE * 256 * ROWS, transcendentals=0, bytes_accessed=16_000_000
        ),
        compiler_params=pltpu.CompilerParams(vmem_limit_bytes=24 << 20),
        name="spread",
    )(
        samples,
        live,
        noise,
        jnp.asarray(chunk_rows(), bf16),
        jnp.asarray(chunk_mask()),
        jnp.asarray(places(), bf16),
    )


def three(v):
    hi = v.astype(bf16).astype(f32)
    mid = (v - hi).astype(bf16).astype(f32)
    return hi, mid, v - hi - mid


UNROLL = 4


def contract(f, block, left_ref, lane):
    left = left_ref[f].reshape(CHUNKS * 8 * ROWS, 256)[:, :DEPTH]
    prod = lax.dot_general(left, block, PLAIN, preferred_element_type=f32)
    prod = prod.reshape(CHUNKS, 4, 4, 8, 128)
    packed = []
    for g in range(CHUNKS):
        acc = jnp.zeros((4, 8, 128), f32)
        for r in range(4):
            moved = pltpu.roll(prod[g, :, r], (32 * r - SITES * g) % 128, 2)
            acc = jnp.where((lane >= 32 * r) & (lane < 32 * r + SITES), moved, acc)
        packed.append(acc)
    cols = [jnp.concatenate([packed[g][q] for g in range(CHUNKS)], axis=0) for q in range(4)]
    return jnp.concatenate(cols, axis=1).astype(bf16)


def walk(ref, base, row0, count, left_ref, z_ref, lane, where, squares):
    def some(s, squares):
        for i in range(UNROLL):
            n = s * UNROLL + i
            f = base + n
            block = ref[n]
            wide = block.astype(f32)
            wide = wide * wide
            squares = squares + jnp.where(where & (f == 0), 0.5 * wide, wide)
            start = pl.multiple_of((row0 + n) * CHUNKS * 8, 16)
            z_ref[pl.ds(start, CHUNKS * 8), :] = contract(f, block, left_ref, lane)
        return squares

    return lax.fori_loop(0, count // UNROLL, some, squares)


def corner():
    where = lax.broadcasted_iota(jnp.int32, (DEPTH, 128), 0) < 2 * SLOTS
    return where & (lax.broadcasted_iota(jnp.int32, (DEPTH, 128), 1) < SITES)


def near_kernel(x_ref, left_ref, own_ref, prev_ref, next_ref, inv_ref, total_ref, sq_ref, z_ref):
    lane = lax.broadcasted_iota(jnp.int32, (4, 8, 128), 2)
    where = corner()
    squares = jnp.zeros((DEPTH, 128), f32)
    x = x_ref[0]
    for ref, off in ((own_ref, 0), (prev_ref, 3), (next_ref, 1)):
        base = lax.rem(x + off, 4) * 8
        squares = walk(ref, base, base, 8, left_ref, z_ref, lane, where, squares)
    far = pl.multiple_of(lax.rem(x + 2, 4) * FAR, 16)
    z_ref[pl.ds(far, FAR), :] = jnp.zeros((FAR, WIDE), bf16)
    sq_ref[...] = squares
    total_ref[...] = lax.dot_general(inv_ref[...], z_ref[...], PLAIN, preferred_element_type=f32)


FAR = 8 * CHUNKS * 8


def near(x, left, own, prev, after, inverse):
    vmem = pl.BlockSpec(memory_space=pltpu.VMEM)
    return pl.pallas_call(
        near_kernel,
        in_specs=[pl.BlockSpec(memory_space=pltpu.SMEM)] + [vmem] * 5,
        out_specs=[vmem] * 2,
        out_shape=[pltpu.VMEM((WIDE, WIDE), f32), pltpu.VMEM((DEPTH, 128), f32)],
        scratch_shapes=[pltpu.VMEM((TALL, WIDE), bf16)],
        compiler_params=pltpu.CompilerParams(vmem_limit_bytes=20 << 20),
        cost_estimate=pl.CostEstimate(
            flops=2 * 24 * 768 * 256 * 128 + 2 * TALL * WIDE * WIDE,
            transcendentals=0,
            bytes_accessed=14_000_000,
        ),
        name="finish_near",
    )(x, left, own, prev, after, inverse)


def far_kernel(
    x_ref, core_ref, left_ref, one_ref, two_ref, inv_ref, total_ref, sq_ref, noise_ref,
    keep_ref, send_ref, z_ref,
):
    lane = lax.broadcasted_iota(jnp.int32, (4, 8, 128), 2)
    where = corner()
    squares = sq_ref[...]
    far = lax.rem(x_ref[0] + 2, 4)
    for h, ref in enumerate((one_ref, two_ref)):
        squares = walk(ref, far * 8 + 4 * h, 4 * h, 4, left_ref, z_ref, lane, where, squares)
    spots = jnp.sum(squares * noise_ref[...], axis=0, keepdims=True) * (2.0 / PERIOD)
    noise = spots
    for g in range(1, CHUNKS):
        noise = noise + pltpu.roll(spots, 128 - SITES * g, 1)
    noise = jnp.where(lax.broadcasted_iota(jnp.int32, (1, 128), 1) < SITES, noise, 0.0)
    noise = jnp.concatenate([noise, jnp.zeros((1, WIDE - 128), f32)], axis=1)
    row = lax.broadcasted_iota(jnp.int32, (32, WIDE), 0)
    tail = jnp.zeros((32, WIDE), f32)
    for n, part in enumerate(three(noise)):
        tail = jnp.where(row == SITES + n, part, tail)
    inv = inv_ref[:, pl.ds(pl.multiple_of(far * FAR, 128), FAR)]
    total = total_ref[...] + lax.dot_general(inv, z_ref[...], PLAIN, preferred_element_type=f32)
    total = (total.T * (2.0 / PERIOD)).reshape(ROWS, 32, WIDE) + tail[None]
    low, high = total[: ROWS // 2, :24], total[ROWS // 2 :, :24]
    second = core_ref[0] == 1
    keep_ref[...] = jnp.where(second, high, low)
    send_ref[...] = jnp.where(second, low, high).astype(bf16)


def finish_far(x, core, left, one, two, inverse, total, squares, column):
    vmem = pl.BlockSpec(memory_space=pltpu.VMEM)
    return pl.pallas_call(
        far_kernel,
        in_specs=[pl.BlockSpec(memory_space=pltpu.SMEM)] * 2 + [vmem] * 7,
        out_specs=[vmem] * 2,
        out_shape=[
            pltpu.VMEM((ROWS // 2, 24, WIDE), f32),
            pltpu.VMEM((ROWS // 2, 24, WIDE), bf16),
        ],
        scratch_shapes=[pltpu.VMEM((FAR, WIDE), bf16)],
        compiler_params=pltpu.CompilerParams(vmem_limit_bytes=20 << 20),
        name="finish_far",
    )(x, core, left, one, two, inverse, total, squares, column)


def other_core(array):
    return lax.ppermute(array, C, [(0, 1), (1, 0)])


def step_by(array, shift):
    n = lax.axis_size(X)
    return lax.ppermute(array, X, [(i, (i + shift) % n) for i in range(n)])


def pair_kernel(keep_ref, came_ref, out_ref):
    total = keep_ref[...] + came_ref[...].astype(f32)
    noise = jnp.sum(total[:, SITES:24], axis=1, keepdims=True)
    row = lax.broadcasted_iota(jnp.int32, total.shape, 1)
    for n, part in enumerate(three(noise)):
        total = jnp.where(row == SITES + n, part, total)
    out_ref[...] = total.astype(bf16)


def pair_of(keep, came):
    vmem = pl.BlockSpec(memory_space=pltpu.VMEM)
    return pl.pallas_call(
        pair_kernel,
        in_specs=[vmem] * 2,
        out_specs=vmem,
        out_shape=pltpu.VMEM(came.shape, bf16),
        compiler_params=pltpu.CompilerParams(vmem_limit_bytes=8 << 20),
        name="pair",
    )(keep, came)


def merge_kernel(core_ref, mine_ref, theirs_ref, out_ref, low_ref, high_ref):
    second = core_ref[0] == 1
    mine, theirs = mine_ref[...].astype(f32), theirs_ref[...].astype(f32)
    low_ref[...] = jnp.where(second, theirs, mine)
    high_ref[...] = jnp.where(second, mine, theirs)
    for q in range(SITES):
        rows = jnp.concatenate([low_ref[:, q, :], high_ref[:, q, :]], axis=0)
        out_ref[q] = rows[:, :STEPS].astype(bf16)


def merge(core, mine, theirs):
    vmem = pl.BlockSpec(memory_space=pltpu.VMEM)
    return pl.pallas_call(
        merge_kernel,
        in_specs=[pl.BlockSpec(memory_space=pltpu.SMEM)] + [vmem] * 2,
        out_specs=vmem,
        out_shape=jax.ShapeDtypeStruct((SITES, ROWS, STEPS), bf16),
        scratch_shapes=[pltpu.VMEM(mine.shape, f32)] * 2,
        compiler_params=pltpu.CompilerParams(vmem_limit_bytes=8 << 20),
        name="merge",
    )(core, mine, theirs)


def total_kernel(got_ref, rep_ref, noise_ref):
    total = jnp.sum(got_ref[...].astype(f32), axis=0)
    rep_ref[...] = jnp.broadcast_to(total.astype(bf16)[None], rep_ref.shape)
    tail = total[16:24, :SITES]
    row = lax.broadcasted_iota(jnp.int32, tail.shape, 0)
    noise_ref[...] = jnp.sum(jnp.where(row >= SITES - 16, tail, 0.0), axis=0, keepdims=True)


def total_of(got):
    vmem = pl.BlockSpec(memory_space=pltpu.VMEM)
    return pl.pallas_call(
        total_kernel,
        in_specs=[vmem],
        out_specs=[vmem] * 2,
        out_shape=[
            pltpu.VMEM(got.shape, bf16),
            jax.ShapeDtypeStruct((1, SITES), f32),
        ],
        compiler_params=pltpu.CompilerParams(vmem_limit_bytes=8 << 20),
        name="total",
    )(got)


def share(array, axis):
    n = lax.axis_size(axis)
    return lax.all_to_all(
        jnp.broadcast_to(array[None], (n, *array.shape)), axis, 0, 0, tiled=True
    )


def payload_of(response, advance_offset, first_bin):
    k_own = first_bin + lax.iota(jnp.int32, BINS)
    turn = (k_own[:, None] * advance_offset[None, :]) % PERIOD
    ang = turn.astype(f32) * (2.0 * math.pi / PERIOD)
    cos, sin = jnp.cos(ang)[:, None, :], jnp.sin(ang)[:, None, :]
    re, im = response[:, 0].astype(f32), response[:, 1].astype(f32)
    turned = jnp.stack([re * cos - im * sin, re * sin + im * cos], axis=1).astype(bf16)
    half = turned.reshape(2 * BINS, SLOTS, SITES)
    half = jnp.pad(half, ((0, CHUNKS * HALVES - 2 * BINS), (0, 0), (0, 0)))
    half = half.reshape(CHUNKS, DEPTH, SITES).transpose(1, 0, 2).reshape(DEPTH, CHUNKS * SITES)
    return jnp.pad(half, ((0, 0), (0, 128 - CHUNKS * SITES)))


def noise_of(slot_sensor, sensor_noise):
    ids = lax.iota(jnp.int32, sensor_noise.shape[0])
    slot_noise = jnp.sum(
        jnp.where(slot_sensor[:, None] == ids[None, :], sensor_noise[None, :], 0.0), axis=1
    )
    return slot_noise[:, None]


def on_device(samples, response, slot_sensor, sensor_noise, advance_offset):
    first_bin = lax.axis_index(FREQ) * BINS
    payload = payload_of(response, advance_offset, first_bin)
    x = lax.axis_index(X).astype(jnp.int32).reshape(1)
    core = lax.axis_index(C).astype(jnp.int32).reshape(1)
    payload, x, core = lax.optimization_barrier((payload, x, core))
    own, slot_sensor, sensor_noise = lax.optimization_barrier(
        (share(payload, Z), slot_sensor, sensor_noise)
    )
    live = (slot_sensor >= 0).astype(bf16)[:, None]
    left, inverse, column = spread(samples, live, noise_of(slot_sensor, sensor_noise))
    prev, after = step_by(own, 1), step_by(own, -1)
    prev, after, left, inverse, column = lax.optimization_barrier(
        (prev, after, left, inverse, column)
    )
    total, squares = near(x, left, own, prev, after, inverse)
    one, two = step_by(prev[:4], 1), step_by(after[4:], -1)
    keep, send = finish_far(x, core, left, one, two, inverse, total, squares, column)
    got = lax.all_to_all(pair_of(keep, other_core(send)), Y, 0, 0, tiled=True)
    copies, noise = total_of(got)
    copies, noise = lax.optimization_barrier((copies, noise.reshape(SITES)))
    mine = lax.all_to_all(copies, Y, 0, 0, tiled=True)
    theirs = other_core(mine)
    outlook = merge(core, mine, theirs).transpose(1, 0, 2)
    return outlook, noise


def solution(mesh):
    torus = Mesh(mesh.devices.reshape(4, 8, 8, 2), (X, Z, Y, C))
    return jax.shard_map(
        on_device,
        mesh=torus,
        in_specs=(P(FREQ, SENS, None), P(FREQ, None, SENS, None), P(SENS), P(), P()),
        out_specs=(P(FREQ, None, None), P()),
        check_vma=False,
    )
```

```python
import math

import jax
import jax.numpy as jnp
import numpy as np
from jax import lax
from jax.experimental import pallas as pl
from jax.experimental.pallas import tpu as pltpu
from jax.sharding import Mesh
from jax.sharding import PartitionSpec as P

KEPT = 448
PERIOD = 2 * KEPT
BINS, SLOTS, SITES, STEPS, ROWS = 14, 40, 21, 420, 16
SOURCES = KEPT // BINS
CHUNKS, HALVES = 6, 5
DEPTH = HALVES * SLOTS
TALL = SOURCES * CHUNKS * 8
WIDE = 512
REST = STEPS - 384
X, Z, Y, C = "freq_0", "freq_1", "sens_0", "sens_1"
FREQ = (X, Z)
SENS = (Y, C)
f32, bf16 = jnp.float32, jnp.bfloat16
PLAIN = (((1,), (0,)), ((), ()))
TURNED = (((1,), (1,)), ((), ()))


def base_table():
    k = np.arange(KEPT)[:, None]
    t = np.arange(STEPS)[None, :]
    a = ((k * t) % PERIOD) * (2.0 * np.pi / PERIOD)
    return np.stack([np.cos(a), -np.sin(a)], axis=1)


def chunk_rows():
    table = base_table().reshape(SOURCES, BINS, 2, STEPS)
    table = np.pad(table, ((0, 0), (0, 2), (0, 0), (0, WIDE - STEPS)))
    parts = [table[:, 5 * g // 2 : 5 * g // 2 + 4] for g in range(CHUNKS)]
    return np.stack(parts, axis=1).swapaxes(2, 3).reshape(TALL, WIDE)


def chunk_mask():
    mask = np.zeros((CHUNKS, 2, 4, 256), np.float32)
    for g in range(CHUNKS):
        for h in range(HALVES):
            half = 5 * g + h
            if half < 2 * BINS:
                mask[g, :, half // 2 - 5 * g // 2, h * SLOTS : (h + 1) * SLOTS] = 1.0
    return mask.reshape(CHUNKS, 8, 256)


def places():
    put = np.zeros((3, 256, 256), np.float32)
    for n in range(3):
        for h in range(HALVES):
            for s in range(SLOTS):
                put[n, 128 * (h % 2) + n * SLOTS + s, h * SLOTS + s] = 1.0
    return put


TRIPLES = -(-ROWS // 3)


def spread_kernel(
    x_ref, live_ref, noise_ref, table_ref, mask_ref, put_ref,
    out_ref, inv_ref, col_ref, xs_ref, both_ref,
):
    xs_ref[...] = jnp.zeros_like(xs_ref)
    for r in range(ROWS):
        at = 128 * (r // 3) + SLOTS * (r % 3)
        xs_ref[at : at + SLOTS, :STEPS] = x_ref[r] * live_ref[...]
    rows = table_ref[...].astype(f32)
    place = lax.broadcasted_iota(jnp.int32, (TALL, WIDE), 0)
    inv_ref[...] = (rows * jnp.where((place == 0) | (place == 4), 0.5, 1.0)).T.astype(bf16)
    for h in range(HALVES):
        col_ref[h * SLOTS : (h + 1) * SLOTS] = noise_ref[...]
    shape = (SOURCES, CHUNKS, 8, 256)
    sign = jnp.where(lax.broadcasted_iota(jnp.int32, shape, 2) < 4, -1.0, 1.0)
    odd = lax.broadcasted_iota(jnp.int32, shape, 1) % 2 == 1

    def transform(t, carry):
        some = xs_ref[pl.ds(pl.multiple_of(256 * t, 256), 256), :]
        d = lax.dot_general(table_ref[...], some, TURNED, preferred_element_type=f32)
        d = d.reshape(shape)
        turned = pltpu.roll(d, 4, 2) * sign
        plain = jnp.where(odd, turned, d).reshape(TALL, 256).astype(bf16)
        turned = jnp.where(odd, d, turned).reshape(TALL, 256).astype(bf16)
        for u in range(2):
            both_ref[2 * t + u, :, :128] = plain[:, 128 * u : 128 * (u + 1)]
            both_ref[2 * t + u, :, 128:] = turned[:, 128 * u : 128 * (u + 1)]
        return carry

    lax.fori_loop(0, TRIPLES // 2, transform, 0)

    def pair(p, carry):
        halves = []
        for j in range(2):
            r = 2 * p + j
            d = lax.dot_general(
                both_ref[r // 3], put_ref[lax.rem(r, 3)], PLAIN, preferred_element_type=f32
            )
            halves.append(d.reshape(shape) * mask_ref[...][None])
        wide = jnp.concatenate(halves, axis=2).astype(bf16)
        out_ref[:, :, pl.ds(pl.multiple_of(16 * p, 16), 16), :] = wide
        return carry

    lax.fori_loop(0, ROWS // 2, pair, 0)


def spread(samples, live, noise):
    vmem = pl.BlockSpec(memory_space=pltpu.VMEM)
    return pl.pallas_call(
        spread_kernel,
        in_specs=[vmem] * 6,
        out_specs=[vmem] * 3,
        out_shape=[
            pltpu.VMEM((SOURCES, CHUNKS, 8 * ROWS, 256), bf16),
            pltpu.VMEM((WIDE, TALL), bf16),
            pltpu.VMEM((DEPTH, 1), f32),
        ],
        scratch_shapes=[
            pltpu.VMEM((TRIPLES * 128, WIDE), bf16),
            pltpu.VMEM((TRIPLES, TALL, 256), bf16),
        ],
        cost_estimate=pl.CostEstimate(
            flops=2 * TALL * WIDE * 256 * ROWS, transcendentals=0, bytes_accessed=16_000_000
        ),
        compiler_params=pltpu.CompilerParams(vmem_limit_bytes=24 << 20),
        name="spread",
    )(
        samples,
        live,
        noise,
        jnp.asarray(chunk_rows(), bf16),
        jnp.asarray(chunk_mask()),
        jnp.asarray(places(), bf16),
    )


def three(v):
    hi = v.astype(bf16).astype(f32)
    mid = (v - hi).astype(bf16).astype(f32)
    return hi, mid, v - hi - mid


UNROLL = 4


def contract(f, block, left_ref, lane):
    left = left_ref[f].reshape(CHUNKS * 8 * ROWS, 256)
    block = jnp.concatenate([block, jnp.zeros((256 - DEPTH, 128), bf16)], axis=0)
    prod = lax.dot_general(left, block, PLAIN, preferred_element_type=f32)
    prod = prod.reshape(CHUNKS, 4, 4, 8, 128)
    packed = []
    for g in range(CHUNKS):
        acc = jnp.zeros((4, 8, 128), f32)
        for r in range(4):
            moved = pltpu.roll(prod[g, :, r], (32 * r - SITES * g) % 128, 2)
            acc = jnp.where((lane >= 32 * r) & (lane < 32 * r + SITES), moved, acc)
        packed.append(acc)
    cols = [jnp.concatenate([packed[g][q] for g in range(CHUNKS)], axis=0) for q in range(4)]
    return jnp.concatenate(cols, axis=1).astype(bf16)


def walk(ref, base, row0, count, left_ref, z_ref, lane, where, squares):
    def some(s, squares):
        for i in range(UNROLL):
            n = s * UNROLL + i
            f = base + n
            block = ref[n]
            wide = block.astype(f32)
            wide = wide * wide
            squares = squares + jnp.where(where & (f == 0), 0.5 * wide, wide)
            start = pl.multiple_of((row0 + n) * CHUNKS * 8, 16)
            z_ref[pl.ds(start, CHUNKS * 8), :] = contract(f, block, left_ref, lane)
        return squares

    return lax.fori_loop(0, count // UNROLL, some, squares)


def corner():
    where = lax.broadcasted_iota(jnp.int32, (DEPTH, 128), 0) < 2 * SLOTS
    return where & (lax.broadcasted_iota(jnp.int32, (DEPTH, 128), 1) < SITES)


def near_kernel(x_ref, left_ref, own_ref, prev_ref, next_ref, inv_ref, total_ref, sq_ref, z_ref):
    lane = lax.broadcasted_iota(jnp.int32, (4, 8, 128), 2)
    where = corner()
    squares = jnp.zeros((DEPTH, 128), f32)
    x = x_ref[0]
    for ref, off in ((own_ref, 0), (prev_ref, 3), (next_ref, 1)):
        base = lax.rem(x + off, 4) * 8
        squares = walk(ref, base, base, 8, left_ref, z_ref, lane, where, squares)
    far = pl.multiple_of(lax.rem(x + 2, 4) * FAR, 16)
    z_ref[pl.ds(far, FAR), :] = jnp.zeros((FAR, WIDE), bf16)
    sq_ref[...] = squares
    total_ref[...] = lax.dot_general(inv_ref[...], z_ref[...], PLAIN, preferred_element_type=f32)


FAR = 8 * CHUNKS * 8


def near(x, left, own, prev, after, inverse):
    vmem = pl.BlockSpec(memory_space=pltpu.VMEM)
    return pl.pallas_call(
        near_kernel,
        in_specs=[pl.BlockSpec(memory_space=pltpu.SMEM)] + [vmem] * 5,
        out_specs=[vmem] * 2,
        out_shape=[pltpu.VMEM((WIDE, WIDE), f32), pltpu.VMEM((DEPTH, 128), f32)],
        scratch_shapes=[pltpu.VMEM((TALL, WIDE), bf16)],
        compiler_params=pltpu.CompilerParams(vmem_limit_bytes=20 << 20),
        cost_estimate=pl.CostEstimate(
            flops=2 * 24 * 768 * 256 * 128 + 2 * TALL * WIDE * WIDE,
            transcendentals=0,
            bytes_accessed=14_000_000,
        ),
        name="finish_near",
    )(x, left, own, prev, after, inverse)


def far_kernel(
    x_ref, core_ref, left_ref, one_ref, two_ref, inv_ref, total_ref, sq_ref, noise_ref,
    keep_ref, send_ref, z_ref,
):
    lane = lax.broadcasted_iota(jnp.int32, (4, 8, 128), 2)
    where = corner()
    squares = sq_ref[...]
    far = lax.rem(x_ref[0] + 2, 4)
    for h, ref in enumerate((one_ref, two_ref)):
        squares = walk(ref, far * 8 + 4 * h, 4 * h, 4, left_ref, z_ref, lane, where, squares)
    spots = jnp.sum(squares * noise_ref[...], axis=0, keepdims=True) * (2.0 / PERIOD)
    noise = spots
    for g in range(1, CHUNKS):
        noise = noise + pltpu.roll(spots, 128 - SITES * g, 1)
    noise = jnp.where(lax.broadcasted_iota(jnp.int32, (1, 128), 1) < SITES, noise, 0.0)
    noise = jnp.concatenate([noise, jnp.zeros((1, WIDE - 128), f32)], axis=1)
    row = lax.broadcasted_iota(jnp.int32, (32, WIDE), 0)
    tail = jnp.zeros((32, WIDE), f32)
    for n, part in enumerate(three(noise)):
        tail = jnp.where(row == SITES + n, part, tail)
    inv = inv_ref[:, pl.ds(pl.multiple_of(far * FAR, 128), FAR)]
    total = total_ref[...] + lax.dot_general(inv, z_ref[...], PLAIN, preferred_element_type=f32)
    total = (total.T * (2.0 / PERIOD)).reshape(ROWS, 32, WIDE) + tail[None]
    rest = total[:, :24, 384:]
    ends = rest[:, :8]
    for n in (1, 2):
        ends += pltpu.roll(rest[:, 8 * n : 8 * n + 8], REST * n, 2)
    total = jnp.concatenate([total[:, :24, 128 * n : 128 * n + 128] for n in range(3)] + [ends], axis=1)
    low, high = total[: ROWS // 2], total[ROWS // 2 :]
    second = core_ref[0] == 1
    keep_ref[...] = jnp.where(second, high, low)
    send_ref[...] = jnp.where(second, low, high).astype(bf16)


def finish_far(x, core, left, one, two, inverse, total, squares, column):
    vmem = pl.BlockSpec(memory_space=pltpu.VMEM)
    return pl.pallas_call(
        far_kernel,
        in_specs=[pl.BlockSpec(memory_space=pltpu.SMEM)] * 2 + [vmem] * 7,
        out_specs=[vmem] * 2,
        out_shape=[
            pltpu.VMEM((ROWS // 2, 80, 128), f32),
            pltpu.VMEM((ROWS // 2, 80, 128), bf16),
        ],
        scratch_shapes=[pltpu.VMEM((FAR, WIDE), bf16)],
        compiler_params=pltpu.CompilerParams(vmem_limit_bytes=20 << 20),
        name="finish_far",
    )(x, core, left, one, two, inverse, total, squares, column)


def other_core(array):
    return lax.ppermute(array, C, [(0, 1), (1, 0)])


def step_by(array, shift):
    n = lax.axis_size(X)
    return lax.ppermute(array, X, [(i, (i + shift) % n) for i in range(n)])


def pair_kernel(keep_ref, came_ref, out_ref):
    total = keep_ref[...] + came_ref[...].astype(f32)
    noise = jnp.sum(total[:, SITES:24], axis=1, keepdims=True)
    row = lax.broadcasted_iota(jnp.int32, total.shape, 1)
    for n, part in enumerate(three(noise)):
        total = jnp.where(row == SITES + n, part, total)
    out_ref[...] = total.astype(bf16)


def pair_of(keep, came):
    vmem = pl.BlockSpec(memory_space=pltpu.VMEM)
    return pl.pallas_call(
        pair_kernel,
        in_specs=[vmem] * 2,
        out_specs=vmem,
        out_shape=pltpu.VMEM(came.shape, bf16),
        compiler_params=pltpu.CompilerParams(vmem_limit_bytes=8 << 20),
        name="pair",
    )(keep, came)


def merge_kernel(core_ref, mine_ref, theirs_ref, out_ref, low_ref, high_ref):
    second = core_ref[0] == 1
    mine, theirs = mine_ref[...].astype(f32), theirs_ref[...].astype(f32)
    low_ref[...] = jnp.where(second, theirs, mine)
    high_ref[...] = jnp.where(second, mine, theirs)
    for q in range(SITES):
        for n in range(4):
            at = 24 * n + q if n < 3 else 72 + q % 8
            rows = jnp.concatenate([low_ref[:, at, :], high_ref[:, at, :]], axis=0)
            if n == 3:
                rows = pltpu.roll(rows, (128 - REST * (q // 8)) % 128, 1)[:, :REST]
            out_ref[q, :, 128 * n : min(128 * n + 128, STEPS)] = rows.astype(bf16)


def merge(core, mine, theirs):
    vmem = pl.BlockSpec(memory_space=pltpu.VMEM)
    return pl.pallas_call(
        merge_kernel,
        in_specs=[pl.BlockSpec(memory_space=pltpu.SMEM)] + [vmem] * 2,
        out_specs=vmem,
        out_shape=jax.ShapeDtypeStruct((SITES, ROWS, STEPS), bf16),
        scratch_shapes=[pltpu.VMEM(mine.shape, f32)] * 2,
        compiler_params=pltpu.CompilerParams(vmem_limit_bytes=8 << 20),
        name="merge",
    )(core, mine, theirs)


def total_kernel(got_ref, rep_ref, noise_ref):
    total = jnp.sum(got_ref[...].astype(f32), axis=0)
    rep_ref[...] = jnp.broadcast_to(total.astype(bf16)[None], rep_ref.shape)
    tail = total[16:24, :SITES]
    row = lax.broadcasted_iota(jnp.int32, tail.shape, 0)
    noise_ref[...] = jnp.sum(jnp.where(row >= SITES - 16, tail, 0.0), axis=0, keepdims=True)


def total_of(got):
    vmem = pl.BlockSpec(memory_space=pltpu.VMEM)
    return pl.pallas_call(
        total_kernel,
        in_specs=[vmem],
        out_specs=[vmem] * 2,
        out_shape=[
            pltpu.VMEM(got.shape, bf16),
            jax.ShapeDtypeStruct((1, SITES), f32),
        ],
        compiler_params=pltpu.CompilerParams(vmem_limit_bytes=8 << 20),
        name="total",
    )(got)


def share(array, axis):
    n = lax.axis_size(axis)
    return lax.all_to_all(
        jnp.broadcast_to(array[None], (n, *array.shape)), axis, 0, 0, tiled=True
    )


def payload_of(response, advance_offset, first_bin):
    k_own = first_bin + lax.iota(jnp.int32, BINS)
    turn = (k_own[:, None] * advance_offset[None, :]) % PERIOD
    ang = turn.astype(f32) * (2.0 * math.pi / PERIOD)
    cos, sin = jnp.cos(ang)[:, None, :], jnp.sin(ang)[:, None, :]
    re, im = response[:, 0].astype(f32), response[:, 1].astype(f32)
    turned = jnp.stack([re * cos - im * sin, re * sin + im * cos], axis=1).astype(bf16)
    half = turned.reshape(2 * BINS, SLOTS, SITES)
    half = jnp.pad(half, ((0, CHUNKS * HALVES - 2 * BINS), (0, 0), (0, 0)))
    half = half.reshape(CHUNKS, DEPTH, SITES).transpose(1, 0, 2).reshape(DEPTH, CHUNKS * SITES)
    return jnp.pad(half, ((0, 0), (0, 128 - CHUNKS * SITES)))


def noise_of(slot_sensor, sensor_noise):
    ids = lax.iota(jnp.int32, sensor_noise.shape[0])
    slot_noise = jnp.sum(
        jnp.where(slot_sensor[:, None] == ids[None, :], sensor_noise[None, :], 0.0), axis=1
    )
    return slot_noise[:, None]


def on_device(samples, response, slot_sensor, sensor_noise, advance_offset):
    first_bin = lax.axis_index(FREQ) * BINS
    payload = payload_of(response, advance_offset, first_bin)
    x = lax.axis_index(X).astype(jnp.int32).reshape(1)
    core = lax.axis_index(C).astype(jnp.int32).reshape(1)
    payload, x, core = lax.optimization_barrier((payload, x, core))
    own, slot_sensor, sensor_noise = lax.optimization_barrier(
        (share(payload, Z), slot_sensor, sensor_noise)
    )
    live = (slot_sensor >= 0).astype(bf16)[:, None]
    left, inverse, column = spread(samples, live, noise_of(slot_sensor, sensor_noise))
    prev, after = step_by(own, 1), step_by(own, -1)
    prev, after, left, inverse, column = lax.optimization_barrier(
        (prev, after, left, inverse, column)
    )
    total, squares = near(x, left, own, prev, after, inverse)
    one, two = step_by(prev[:4], 1), step_by(after[4:], -1)
    keep, send = finish_far(x, core, left, one, two, inverse, total, squares, column)
    got = lax.all_to_all(pair_of(keep, other_core(send)), Y, 0, 0, tiled=True)
    copies, noise = total_of(got)
    copies, noise = lax.optimization_barrier((copies, noise.reshape(SITES)))
    mine = lax.all_to_all(copies, Y, 0, 0, tiled=True)
    theirs = other_core(mine)
    outlook = merge(core, mine, theirs).transpose(1, 0, 2)
    return outlook, noise


def solution(mesh):
    torus = Mesh(mesh.devices.reshape(4, 8, 8, 2), (X, Z, Y, C))
    return jax.shard_map(
        on_device,
        mesh=torus,
        in_specs=(P(FREQ, SENS, None), P(FREQ, None, SENS, None), P(SENS), P(), P()),
        out_specs=(P(FREQ, None, None), P()),
        check_vma=False,
    )
```

```python
import math

import jax
import jax.numpy as jnp
import numpy as np
from jax import lax
from jax.experimental import pallas as pl
from jax.experimental.pallas import tpu as pltpu
from jax.sharding import Mesh
from jax.sharding import PartitionSpec as P

KEPT = 448
PERIOD = 2 * KEPT
BINS, SLOTS, SITES, STEPS, ROWS = 14, 40, 21, 420, 16
SOURCES = KEPT // BINS
CHUNKS, HALVES = 6, 5
DEPTH = HALVES * SLOTS
TALL = SOURCES * CHUNKS * 8
WIDE = 512
REST = STEPS - 384
X, Z, Y, C = "freq_0", "freq_1", "sens_0", "sens_1"
FREQ = (X, Z)
SENS = (Y, C)
f32, bf16 = jnp.float32, jnp.bfloat16
PLAIN = (((1,), (0,)), ((), ()))
TURNED = (((1,), (1,)), ((), ()))


def base_table():
    k = np.arange(KEPT)[:, None]
    t = np.arange(STEPS)[None, :]
    a = ((k * t) % PERIOD) * (2.0 * np.pi / PERIOD)
    return np.stack([np.cos(a), -np.sin(a)], axis=1)


def chunk_rows():
    table = base_table().reshape(SOURCES, BINS, 2, STEPS)
    table = np.pad(table, ((0, 0), (0, 2), (0, 0), (0, WIDE - STEPS)))
    parts = [table[:, 5 * g // 2 : 5 * g // 2 + 4] for g in range(CHUNKS)]
    return np.stack(parts, axis=1).swapaxes(2, 3).reshape(TALL, WIDE)


def chunk_mask():
    mask = np.zeros((CHUNKS, 2, 4, 256), np.float32)
    for g in range(CHUNKS):
        for h in range(HALVES):
            half = 5 * g + h
            if half < 2 * BINS:
                mask[g, :, half // 2 - 5 * g // 2, h * SLOTS : (h + 1) * SLOTS] = 1.0
    return mask.reshape(CHUNKS, 8, 256)


TRIPLES = -(-ROWS // 3)


def spread_kernel(
    x_ref, live_ref, noise_ref, table_ref, mask_ref,
    out_ref, inv_ref, col_ref, xs_ref, both_ref, put_ref,
):
    xs_ref[...] = jnp.zeros_like(xs_ref)
    for r in range(ROWS):
        at = 128 * (r // 3) + SLOTS * (r % 3)
        xs_ref[at : at + SLOTS, :STEPS] = x_ref[r] * live_ref[...]
    rows = table_ref[...].astype(f32)
    place = lax.broadcasted_iota(jnp.int32, (TALL, WIDE), 0)
    inv_ref[...] = (rows * jnp.where((place == 0) | (place == 4), 0.5, 1.0)).T.astype(bf16)
    for h in range(HALVES):
        col_ref[h * SLOTS : (h + 1) * SLOTS] = noise_ref[...]
    down = lax.broadcasted_iota(jnp.int32, (256, 256), 0)
    lane = lax.broadcasted_iota(jnp.int32, (256, 256), 1)
    source = lane
    for h in range(1, HALVES):
        source += jnp.where(lane >= SLOTS * h, (128 if h % 2 else -128) - SLOTS, 0)
    for n in range(3):
        put = jnp.where((down == source + SLOTS * n) & (lane < DEPTH), 1.0, 0.0)
        put_ref[n] = put.astype(bf16)
    shape = (SOURCES, CHUNKS, 8, 256)
    sign = jnp.where(lax.broadcasted_iota(jnp.int32, shape, 2) < 4, -1.0, 1.0)
    odd = lax.broadcasted_iota(jnp.int32, shape, 1) % 2 == 1

    def transform(t, carry):
        some = xs_ref[pl.ds(pl.multiple_of(256 * t, 256), 256), :]
        d = lax.dot_general(table_ref[...], some, TURNED, preferred_element_type=f32)
        d = d.reshape(shape)
        turned = pltpu.roll(d, 4, 2) * sign
        plain = jnp.where(odd, turned, d).reshape(TALL, 256).astype(bf16)
        turned = jnp.where(odd, d, turned).reshape(TALL, 256).astype(bf16)
        for u in range(2):
            both_ref[2 * t + u, :, :128] = plain[:, 128 * u : 128 * (u + 1)]
            both_ref[2 * t + u, :, 128:] = turned[:, 128 * u : 128 * (u + 1)]
        return carry

    lax.fori_loop(0, TRIPLES // 2, transform, 0)

    def pair(p, carry):
        halves = []
        for j in range(2):
            r = 2 * p + j
            d = lax.dot_general(
                both_ref[r // 3], put_ref[lax.rem(r, 3)], PLAIN, preferred_element_type=f32
            )
            halves.append(d.reshape(shape) * mask_ref[...][None])
        wide = jnp.concatenate(halves, axis=2).astype(bf16)
        out_ref[:, :, pl.ds(pl.multiple_of(16 * p, 16), 16), :] = wide
        return carry

    lax.fori_loop(0, ROWS // 2, pair, 0)


def spread(samples, live, noise):
    vmem = pl.BlockSpec(memory_space=pltpu.VMEM)
    return pl.pallas_call(
        spread_kernel,
        in_specs=[vmem] * 5,
        out_specs=[vmem] * 3,
        out_shape=[
            pltpu.VMEM((SOURCES, CHUNKS, 8 * ROWS, 256), bf16),
            pltpu.VMEM((WIDE, TALL), bf16),
            pltpu.VMEM((DEPTH, 1), f32),
        ],
        scratch_shapes=[
            pltpu.VMEM((TRIPLES * 128, WIDE), bf16),
            pltpu.VMEM((TRIPLES, TALL, 256), bf16),
            pltpu.VMEM((3, 256, 256), bf16),
        ],
        cost_estimate=pl.CostEstimate(
            flops=2 * TALL * WIDE * 256 * ROWS, transcendentals=0, bytes_accessed=16_000_000
        ),
        compiler_params=pltpu.CompilerParams(vmem_limit_bytes=24 << 20),
        name="spread",
    )(
        samples,
        live,
        noise,
        jnp.asarray(chunk_rows(), bf16),
        jnp.asarray(chunk_mask()),
    )


def three(v):
    hi = v.astype(bf16).astype(f32)
    mid = (v - hi).astype(bf16).astype(f32)
    return hi, mid, v - hi - mid


UNROLL = 4


def contract(f, block, left_ref, lane):
    left = left_ref[f].reshape(CHUNKS * 8 * ROWS, 256)
    block = jnp.concatenate([block, jnp.zeros((256 - DEPTH, 128), bf16)], axis=0)
    prod = lax.dot_general(left, block, PLAIN, preferred_element_type=f32)
    prod = prod.reshape(CHUNKS, 4, 4, 8, 128)
    packed = []
    for g in range(CHUNKS):
        acc = jnp.zeros((4, 8, 128), f32)
        for r in range(4):
            moved = pltpu.roll(prod[g, :, r], (32 * r - SITES * g) % 128, 2)
            acc = jnp.where((lane >= 32 * r) & (lane < 32 * r + SITES), moved, acc)
        packed.append(acc)
    cols = [jnp.concatenate([packed[g][q] for g in range(CHUNKS)], axis=0) for q in range(4)]
    return jnp.concatenate(cols, axis=1).astype(bf16)


def walk(ref, base, row0, count, left_ref, z_ref, lane, where, squares):
    def some(s, squares):
        for i in range(UNROLL):
            n = s * UNROLL + i
            f = base + n
            block = ref[n]
            wide = block.astype(f32)
            wide = wide * wide
            squares = squares + jnp.where(where & (f == 0), 0.5 * wide, wide)
            start = pl.multiple_of((row0 + n) * CHUNKS * 8, 16)
            z_ref[pl.ds(start, CHUNKS * 8), :] = contract(f, block, left_ref, lane)
        return squares

    return lax.fori_loop(0, count // UNROLL, some, squares)


def corner():
    where = lax.broadcasted_iota(jnp.int32, (DEPTH, 128), 0) < 2 * SLOTS
    return where & (lax.broadcasted_iota(jnp.int32, (DEPTH, 128), 1) < SITES)


def near_kernel(x_ref, left_ref, own_ref, prev_ref, next_ref, inv_ref, total_ref, sq_ref, z_ref):
    lane = lax.broadcasted_iota(jnp.int32, (4, 8, 128), 2)
    where = corner()
    squares = jnp.zeros((DEPTH, 128), f32)
    x = x_ref[0]
    for ref, off in ((own_ref, 0), (prev_ref, 3), (next_ref, 1)):
        base = lax.rem(x + off, 4) * 8
        squares = walk(ref, base, base, 8, left_ref, z_ref, lane, where, squares)
    far = pl.multiple_of(lax.rem(x + 2, 4) * FAR, 16)
    z_ref[pl.ds(far, FAR), :] = jnp.zeros((FAR, WIDE), bf16)
    sq_ref[...] = squares
    total_ref[...] = lax.dot_general(inv_ref[...], z_ref[...], PLAIN, preferred_element_type=f32)


FAR = 8 * CHUNKS * 8


def near(x, left, own, prev, after, inverse):
    vmem = pl.BlockSpec(memory_space=pltpu.VMEM)
    return pl.pallas_call(
        near_kernel,
        in_specs=[pl.BlockSpec(memory_space=pltpu.SMEM)] + [vmem] * 5,
        out_specs=[vmem] * 2,
        out_shape=[pltpu.VMEM((WIDE, WIDE), f32), pltpu.VMEM((DEPTH, 128), f32)],
        scratch_shapes=[pltpu.VMEM((TALL, WIDE), bf16)],
        compiler_params=pltpu.CompilerParams(vmem_limit_bytes=20 << 20),
        cost_estimate=pl.CostEstimate(
            flops=2 * 24 * 768 * 256 * 128 + 2 * TALL * WIDE * WIDE,
            transcendentals=0,
            bytes_accessed=14_000_000,
        ),
        name="finish_near",
    )(x, left, own, prev, after, inverse)


def far_kernel(
    x_ref, core_ref, left_ref, one_ref, two_ref, inv_ref, total_ref, sq_ref, noise_ref,
    keep_ref, send_ref, z_ref,
):
    lane = lax.broadcasted_iota(jnp.int32, (4, 8, 128), 2)
    where = corner()
    squares = sq_ref[...]
    far = lax.rem(x_ref[0] + 2, 4)
    for h, ref in enumerate((one_ref, two_ref)):
        squares = walk(ref, far * 8 + 4 * h, 4 * h, 4, left_ref, z_ref, lane, where, squares)
    spots = jnp.sum(squares * noise_ref[...], axis=0, keepdims=True) * (2.0 / PERIOD)
    noise = spots
    for g in range(1, CHUNKS):
        noise = noise + pltpu.roll(spots, 128 - SITES * g, 1)
    noise = jnp.where(lax.broadcasted_iota(jnp.int32, (1, 128), 1) < SITES, noise, 0.0)
    noise = jnp.concatenate([noise, jnp.zeros((1, WIDE - 128), f32)], axis=1)
    row = lax.broadcasted_iota(jnp.int32, (32, WIDE), 0)
    tail = jnp.zeros((32, WIDE), f32)
    for n, part in enumerate(three(noise)):
        tail = jnp.where(row == SITES + n, part, tail)
    inv = inv_ref[:, pl.ds(pl.multiple_of(far * FAR, 128), FAR)]
    total = total_ref[...] + lax.dot_general(inv, z_ref[...], PLAIN, preferred_element_type=f32)
    total = (total.T * (2.0 / PERIOD)).reshape(ROWS, 32, WIDE) + tail[None]
    rest = total[:, :24, 384:]
    ends = rest[:, :8]
    for n in (1, 2):
        ends += pltpu.roll(rest[:, 8 * n : 8 * n + 8], REST * n, 2)
    total = jnp.concatenate([total[:, :24, 128 * n : 128 * n + 128] for n in range(3)] + [ends], axis=1)
    low, high = total[: ROWS // 2], total[ROWS // 2 :]
    second = core_ref[0] == 1
    keep_ref[...] = jnp.where(second, high, low)
    send_ref[...] = jnp.where(second, low, high).astype(bf16)


def finish_far(x, core, left, one, two, inverse, total, squares, column):
    vmem = pl.BlockSpec(memory_space=pltpu.VMEM)
    return pl.pallas_call(
        far_kernel,
        in_specs=[pl.BlockSpec(memory_space=pltpu.SMEM)] * 2 + [vmem] * 7,
        out_specs=[vmem] * 2,
        out_shape=[
            pltpu.VMEM((ROWS // 2, 80, 128), f32),
            pltpu.VMEM((ROWS // 2, 80, 128), bf16),
        ],
        scratch_shapes=[pltpu.VMEM((FAR, WIDE), bf16)],
        compiler_params=pltpu.CompilerParams(vmem_limit_bytes=20 << 20),
        name="finish_far",
    )(x, core, left, one, two, inverse, total, squares, column)


def other_core(array):
    return lax.ppermute(array, C, [(0, 1), (1, 0)])


def step_by(array, shift):
    n = lax.axis_size(X)
    return lax.ppermute(array, X, [(i, (i + shift) % n) for i in range(n)])


def pair_kernel(keep_ref, came_ref, out_ref):
    total = keep_ref[...] + came_ref[...].astype(f32)
    noise = jnp.sum(total[:, SITES:24], axis=1, keepdims=True)
    row = lax.broadcasted_iota(jnp.int32, total.shape, 1)
    for n, part in enumerate(three(noise)):
        total = jnp.where(row == SITES + n, part, total)
    out_ref[...] = total.astype(bf16)


def pair_of(keep, came):
    vmem = pl.BlockSpec(memory_space=pltpu.VMEM)
    return pl.pallas_call(
        pair_kernel,
        in_specs=[vmem] * 2,
        out_specs=vmem,
        out_shape=pltpu.VMEM(came.shape, bf16),
        compiler_params=pltpu.CompilerParams(vmem_limit_bytes=8 << 20),
        name="pair",
    )(keep, came)


def merge_kernel(core_ref, mine_ref, theirs_ref, out_ref, low_ref, high_ref):
    second = core_ref[0] == 1
    mine, theirs = mine_ref[...].astype(f32), theirs_ref[...].astype(f32)
    low_ref[...] = jnp.where(second, theirs, mine)
    high_ref[...] = jnp.where(second, mine, theirs)
    for q in range(SITES):
        for n in range(4):
            at = 24 * n + q if n < 3 else 72 + q % 8
            rows = jnp.concatenate([low_ref[:, at, :], high_ref[:, at, :]], axis=0)
            if n == 3:
                rows = pltpu.roll(rows, (128 - REST * (q // 8)) % 128, 1)[:, :REST]
            out_ref[q, :, 128 * n : min(128 * n + 128, STEPS)] = rows.astype(bf16)


def merge(core, mine, theirs):
    vmem = pl.BlockSpec(memory_space=pltpu.VMEM)
    return pl.pallas_call(
        merge_kernel,
        in_specs=[pl.BlockSpec(memory_space=pltpu.SMEM)] + [vmem] * 2,
        out_specs=vmem,
        out_shape=jax.ShapeDtypeStruct((SITES, ROWS, STEPS), bf16),
        scratch_shapes=[pltpu.VMEM(mine.shape, f32)] * 2,
        compiler_params=pltpu.CompilerParams(vmem_limit_bytes=8 << 20),
        name="merge",
    )(core, mine, theirs)


def total_kernel(got_ref, rep_ref, noise_ref):
    total = jnp.sum(got_ref[...].astype(f32), axis=0)
    rep_ref[...] = jnp.broadcast_to(total.astype(bf16)[None], rep_ref.shape)
    tail = total[16:24, :SITES]
    row = lax.broadcasted_iota(jnp.int32, tail.shape, 0)
    noise_ref[...] = jnp.sum(jnp.where(row >= SITES - 16, tail, 0.0), axis=0, keepdims=True)


def total_of(got):
    vmem = pl.BlockSpec(memory_space=pltpu.VMEM)
    return pl.pallas_call(
        total_kernel,
        in_specs=[vmem],
        out_specs=[vmem] * 2,
        out_shape=[
            pltpu.VMEM(got.shape, bf16),
            jax.ShapeDtypeStruct((1, SITES), f32),
        ],
        compiler_params=pltpu.CompilerParams(vmem_limit_bytes=8 << 20),
        name="total",
    )(got)


def turn_kernel(bin_ref, lead_ref, raw_ref, rep_ref):
    w = raw_ref[...].astype(f32).reshape(HALVES, SLOTS, 128)
    lane = lax.broadcasted_iota(jnp.int32, (1, 128), 1)
    chunk = jnp.zeros((1, 128), jnp.int32)
    for g in range(1, CHUNKS):
        chunk += (lane >= SITES * g).astype(jnp.int32)
    lead = jnp.concatenate([lead_ref[...].astype(f32), jnp.zeros((1, 128 - SITES), f32)], axis=1)
    leads = lead
    for g in range(1, CHUNKS):
        leads = leads + pltpu.roll(lead, SITES * g, 1)
    outs = []
    for h in range(HALVES):
        half = HALVES * chunk + h
        real = half % 2 == 0
        turn = (bin_ref[0] + half // 2).astype(f32) * leads
        turn = turn - PERIOD * jnp.floor(turn * (1.0 / PERIOD))
        turn = jnp.where(turn < 0, turn + PERIOD, jnp.where(turn >= PERIOD, turn - PERIOD, turn))
        angle = turn * (2.0 * math.pi / PERIOD)
        cos, sin = jnp.cos(angle), jnp.sin(angle)
        above = w[h + 1] if h < HALVES - 1 else pltpu.roll(w[0], 128 - SITES, 1)
        below = w[h - 1] if h > 0 else pltpu.roll(w[HALVES - 1], SITES, 1)
        other = jnp.where(real, above, below)
        outs.append(w[h] * cos + other * jnp.where(real, -sin, sin))
    out = jnp.concatenate(outs, axis=0).astype(bf16)
    rep_ref[...] = jnp.broadcast_to(out[None], rep_ref.shape)


def copies_of(response, advance_offset, first_bin):
    half = response.reshape(2 * BINS, SLOTS, SITES)
    half = jnp.pad(half, ((0, CHUNKS * HALVES - 2 * BINS), (0, 0), (0, 0)))
    half = half.reshape(CHUNKS, DEPTH, SITES).transpose(1, 0, 2).reshape(DEPTH, CHUNKS * SITES)
    half = jnp.pad(half, ((0, 0), (0, 128 - CHUNKS * SITES)))
    vmem = pl.BlockSpec(memory_space=pltpu.VMEM)
    return pl.pallas_call(
        turn_kernel,
        in_specs=[pl.BlockSpec(memory_space=pltpu.SMEM)] + [vmem] * 2,
        out_specs=vmem,
        out_shape=pltpu.VMEM((8, DEPTH, 128), bf16),
        compiler_params=pltpu.CompilerParams(vmem_limit_bytes=8 << 20),
        name="turn",
    )(jnp.asarray(first_bin, jnp.int32).reshape(1), advance_offset.reshape(1, SITES), half)


def noise_of(slot_sensor, sensor_noise):
    ids = lax.iota(jnp.int32, sensor_noise.shape[0])
    slot_noise = jnp.sum(
        jnp.where(slot_sensor[:, None] == ids[None, :], sensor_noise[None, :], 0.0), axis=1
    )
    return slot_noise[:, None]


def on_device(samples, response, slot_sensor, sensor_noise, advance_offset):
    first_bin = lax.axis_index(FREQ) * BINS
    copies = copies_of(response, advance_offset, first_bin)
    x = lax.axis_index(X).astype(jnp.int32).reshape(1)
    core = lax.axis_index(C).astype(jnp.int32).reshape(1)
    copies, x, core = lax.optimization_barrier((copies, x, core))
    own, slot_sensor, sensor_noise = lax.optimization_barrier(
        (lax.all_to_all(copies, Z, 0, 0, tiled=True), slot_sensor, sensor_noise)
    )
    live = (slot_sensor >= 0).astype(bf16)[:, None]
    left, inverse, column = spread(samples, live, noise_of(slot_sensor, sensor_noise))
    prev, after = step_by(own, 1), step_by(own, -1)
    prev, after, left, inverse, column = lax.optimization_barrier(
        (prev, after, left, inverse, column)
    )
    total, squares = near(x, left, own, prev, after, inverse)
    one, two = step_by(prev[:4], 1), step_by(after[4:], -1)
    keep, send = finish_far(x, core, left, one, two, inverse, total, squares, column)
    got = lax.all_to_all(pair_of(keep, other_core(send)), Y, 0, 0, tiled=True)
    copies, noise = total_of(got)
    copies, noise = lax.optimization_barrier((copies, noise.reshape(SITES)))
    mine = lax.all_to_all(copies, Y, 0, 0, tiled=True)
    theirs = other_core(mine)
    outlook = merge(core, mine, theirs).transpose(1, 0, 2)
    return outlook, noise


def solution(mesh):
    torus = Mesh(mesh.devices.reshape(4, 8, 8, 2), (X, Z, Y, C))
    return jax.shard_map(
        on_device,
        mesh=torus,
        in_specs=(P(FREQ, SENS, None), P(FREQ, None, SENS, None), P(SENS), P(), P()),
        out_specs=(P(FREQ, None, None), P()),
        check_vma=False,
    )
```

```python
import math

import jax
import jax.numpy as jnp
import numpy as np
from jax import lax
from jax.experimental import pallas as pl
from jax.experimental.pallas import tpu as pltpu
from jax.sharding import Mesh
from jax.sharding import PartitionSpec as P

KEPT = 448
PERIOD = 2 * KEPT
BINS, SLOTS, SITES, STEPS, ROWS = 14, 40, 21, 420, 16
SOURCES = KEPT // BINS
CHUNKS, HALVES = 6, 5
DEPTH = HALVES * SLOTS
TALL = SOURCES * CHUNKS * 8
WIDE = 512
REST = STEPS - 384
X, Z, Y, C = "freq_0", "freq_1", "sens_0", "sens_1"
FREQ = (X, Z)
SENS = (Y, C)
f32, bf16 = jnp.float32, jnp.bfloat16
PLAIN = (((1,), (0,)), ((), ()))
TURNED = (((1,), (1,)), ((), ()))


def base_table():
    k = np.arange(KEPT)[:, None]
    t = np.arange(STEPS)[None, :]
    a = ((k * t) % PERIOD) * (2.0 * np.pi / PERIOD)
    return np.stack([np.cos(a), -np.sin(a)], axis=1)


def chunk_rows():
    table = base_table().reshape(SOURCES, BINS, 2, STEPS)
    table = np.pad(table, ((0, 0), (0, 2), (0, 0), (0, WIDE - STEPS)))
    parts = [table[:, 5 * g // 2 : 5 * g // 2 + 4] for g in range(CHUNKS)]
    return np.stack(parts, axis=1).swapaxes(2, 3).reshape(TALL, WIDE)


def chunk_mask():
    mask = np.zeros((CHUNKS, 2, 4, 256), np.float32)
    for g in range(CHUNKS):
        for h in range(HALVES):
            half = 5 * g + h
            if half < 2 * BINS:
                mask[g, :, half // 2 - 5 * g // 2, h * SLOTS : (h + 1) * SLOTS] = 1.0
    return mask.reshape(CHUNKS, 8, 256)


TRIPLES = -(-ROWS // 3)


def spread_kernel(
    x_ref, live_ref, noise_ref, table_ref, mask_ref,
    out_ref, inv_ref, col_ref, xs_ref, both_ref, put_ref,
):
    xs_ref[...] = jnp.zeros_like(xs_ref)
    for r in range(ROWS):
        at = 128 * (r // 3) + SLOTS * (r % 3)
        xs_ref[at : at + SLOTS, :STEPS] = x_ref[r] * live_ref[...]
    rows = table_ref[...].astype(f32)
    place = lax.broadcasted_iota(jnp.int32, (TALL, WIDE), 0)
    inv_ref[...] = (rows * jnp.where((place == 0) | (place == 4), 0.5, 1.0)).T.astype(bf16)
    for h in range(HALVES):
        col_ref[h * SLOTS : (h + 1) * SLOTS] = noise_ref[...]
    down = lax.broadcasted_iota(jnp.int32, (256, 256), 0)
    lane = lax.broadcasted_iota(jnp.int32, (256, 256), 1)
    source = lane
    for h in range(1, HALVES):
        source += jnp.where(lane >= SLOTS * h, (128 if h % 2 else -128) - SLOTS, 0)
    for n in range(3):
        put = jnp.where((down == source + SLOTS * n) & (lane < DEPTH), 1.0, 0.0)
        put_ref[n] = put.astype(bf16)
    shape = (SOURCES, CHUNKS, 8, 256)
    sign = jnp.where(lax.broadcasted_iota(jnp.int32, shape, 2) < 4, -1.0, 1.0)
    odd = lax.broadcasted_iota(jnp.int32, shape, 1) % 2 == 1

    def transform(t, carry):
        some = xs_ref[pl.ds(pl.multiple_of(256 * t, 256), 256), :]
        d = lax.dot_general(table_ref[...], some, TURNED, preferred_element_type=f32)
        d = d.reshape(shape)
        turned = pltpu.roll(d, 4, 2) * sign
        plain = jnp.where(odd, turned, d).reshape(TALL, 256).astype(bf16)
        turned = jnp.where(odd, d, turned).reshape(TALL, 256).astype(bf16)
        for u in range(2):
            both_ref[2 * t + u, :, :128] = plain[:, 128 * u : 128 * (u + 1)]
            both_ref[2 * t + u, :, 128:] = turned[:, 128 * u : 128 * (u + 1)]
        return carry

    lax.fori_loop(0, TRIPLES // 2, transform, 0)

    def pair(p, carry):
        halves = []
        for j in range(2):
            r = 2 * p + j
            d = lax.dot_general(
                both_ref[r // 3], put_ref[lax.rem(r, 3)], PLAIN, preferred_element_type=f32
            )
            halves.append(d.reshape(shape) * mask_ref[...][None])
        wide = jnp.concatenate(halves, axis=2).astype(bf16)
        out_ref[:, :, pl.ds(pl.multiple_of(16 * p, 16), 16), :] = wide
        return carry

    lax.fori_loop(0, ROWS // 2, pair, 0)


def spread(samples, live, noise):
    vmem = pl.BlockSpec(memory_space=pltpu.VMEM)
    return pl.pallas_call(
        spread_kernel,
        in_specs=[vmem] * 5,
        out_specs=[vmem] * 3,
        out_shape=[
            pltpu.VMEM((SOURCES, CHUNKS, 8 * ROWS, 256), bf16),
            pltpu.VMEM((WIDE, TALL), bf16),
            pltpu.VMEM((DEPTH, 1), f32),
        ],
        scratch_shapes=[
            pltpu.VMEM((TRIPLES * 128, WIDE), bf16),
            pltpu.VMEM((TRIPLES, TALL, 256), bf16),
            pltpu.VMEM((3, 256, 256), bf16),
        ],
        cost_estimate=pl.CostEstimate(
            flops=2 * TALL * WIDE * 256 * ROWS, transcendentals=0, bytes_accessed=16_000_000
        ),
        compiler_params=pltpu.CompilerParams(vmem_limit_bytes=24 << 20),
        name="spread",
    )(
        samples,
        live,
        noise,
        jnp.asarray(chunk_rows(), bf16),
        jnp.asarray(chunk_mask()),
    )


def three(v):
    hi = v.astype(bf16).astype(f32)
    mid = (v - hi).astype(bf16).astype(f32)
    return hi, mid, v - hi - mid


UNROLL = 4


def contract(f, block, left_ref, lane):
    left = left_ref[f].reshape(CHUNKS * 8 * ROWS, 256)
    block = jnp.concatenate([block, jnp.zeros((256 - DEPTH, 128), bf16)], axis=0)
    prod = lax.dot_general(left, block, PLAIN, preferred_element_type=f32)
    prod = prod.reshape(CHUNKS, 4, 4, 8, 128)
    packed = []
    for g in range(CHUNKS):
        acc = jnp.zeros((4, 8, 128), f32)
        for r in range(4):
            moved = pltpu.roll(prod[g, :, r], (32 * r - SITES * g) % 128, 2)
            acc = jnp.where((lane >= 32 * r) & (lane < 32 * r + SITES), moved, acc)
        packed.append(acc)
    cols = [jnp.concatenate([packed[g][q] for g in range(CHUNKS)], axis=0) for q in range(4)]
    return jnp.concatenate(cols, axis=1).astype(bf16)


def walk(ref, base, row0, count, left_ref, z_ref, lane, where, squares):
    def some(s, squares):
        for i in range(UNROLL):
            n = s * UNROLL + i
            f = base + n
            block = ref[n]
            wide = block.astype(f32)
            wide = wide * wide
            squares = squares + jnp.where(where & (f == 0), 0.5 * wide, wide)
            start = pl.multiple_of((row0 + n) * CHUNKS * 8, 16)
            z_ref[pl.ds(start, CHUNKS * 8), :] = contract(f, block, left_ref, lane)
        return squares

    return lax.fori_loop(0, count // UNROLL, some, squares)


def corner():
    where = lax.broadcasted_iota(jnp.int32, (DEPTH, 128), 0) < 2 * SLOTS
    return where & (lax.broadcasted_iota(jnp.int32, (DEPTH, 128), 1) < SITES)


def near_kernel(x_ref, left_ref, own_ref, prev_ref, next_ref, inv_ref, total_ref, sq_ref, z_ref):
    lane = lax.broadcasted_iota(jnp.int32, (4, 8, 128), 2)
    where = corner()
    squares = jnp.zeros((DEPTH, 128), f32)
    x = x_ref[0]
    for ref, off in ((own_ref, 0), (prev_ref, 3), (next_ref, 1)):
        base = lax.rem(x + off, 4) * 8
        squares = walk(ref, base, base, 8, left_ref, z_ref, lane, where, squares)
    far = pl.multiple_of(lax.rem(x + 2, 4) * FAR, 16)
    z_ref[pl.ds(far, FAR), :] = jnp.zeros((FAR, WIDE), bf16)
    sq_ref[...] = squares
    total_ref[...] = lax.dot_general(inv_ref[...], z_ref[...], PLAIN, preferred_element_type=f32)


FAR = 8 * CHUNKS * 8


def near(x, left, own, prev, after, inverse):
    vmem = pl.BlockSpec(memory_space=pltpu.VMEM)
    return pl.pallas_call(
        near_kernel,
        in_specs=[pl.BlockSpec(memory_space=pltpu.SMEM)] + [vmem] * 5,
        out_specs=[vmem] * 2,
        out_shape=[pltpu.VMEM((WIDE, WIDE), f32), pltpu.VMEM((DEPTH, 128), f32)],
        scratch_shapes=[pltpu.VMEM((TALL, WIDE), bf16)],
        compiler_params=pltpu.CompilerParams(vmem_limit_bytes=20 << 20),
        cost_estimate=pl.CostEstimate(
            flops=2 * 24 * 768 * 256 * 128 + 2 * TALL * WIDE * WIDE,
            transcendentals=0,
            bytes_accessed=14_000_000,
        ),
        name="finish_near",
    )(x, left, own, prev, after, inverse)


def far_kernel(
    x_ref, core_ref, left_ref, one_ref, two_ref, inv_ref, total_ref, sq_ref, noise_ref,
    keep_ref, send_ref, z_ref,
):
    lane = lax.broadcasted_iota(jnp.int32, (4, 8, 128), 2)
    where = corner()
    squares = sq_ref[...]
    far = lax.rem(x_ref[0] + 2, 4)
    for h, ref in enumerate((one_ref, two_ref)):
        squares = walk(ref, far * 8 + 4 * h, 4 * h, 4, left_ref, z_ref, lane, where, squares)
    spots = jnp.sum(squares * noise_ref[...], axis=0, keepdims=True) * (2.0 / PERIOD)
    noise = spots
    for g in range(1, CHUNKS):
        noise = noise + pltpu.roll(spots, 128 - SITES * g, 1)
    noise = jnp.where(lax.broadcasted_iota(jnp.int32, (1, 128), 1) < SITES, noise, 0.0)
    noise = jnp.concatenate([noise, jnp.zeros((1, WIDE - 128), f32)], axis=1)
    row = lax.broadcasted_iota(jnp.int32, (32, WIDE), 0)
    tail = jnp.zeros((32, WIDE), f32)
    for n, part in enumerate(three(noise)):
        tail = jnp.where(row == SITES + n, part, tail)
    inv = inv_ref[:, pl.ds(pl.multiple_of(far * FAR, 128), FAR)]
    total = total_ref[...] + lax.dot_general(inv, z_ref[...], PLAIN, preferred_element_type=f32)
    total = (total.T * (2.0 / PERIOD)).reshape(ROWS, 32, WIDE) + tail[None]
    rest = total[:, :24, 384:]
    ends = rest[:, :8]
    for n in (1, 2):
        ends += pltpu.roll(rest[:, 8 * n : 8 * n + 8], REST * n, 2)
    total = jnp.concatenate([total[:, :24, 128 * n : 128 * n + 128] for n in range(3)] + [ends], axis=1)
    low, high = total[: ROWS // 2], total[ROWS // 2 :]
    second = core_ref[0] == 1
    keep_ref[...] = jnp.where(second, high, low)
    send_ref[...] = jnp.where(second, low, high).astype(bf16)


def finish_far(x, core, left, one, two, inverse, total, squares, column):
    vmem = pl.BlockSpec(memory_space=pltpu.VMEM)
    return pl.pallas_call(
        far_kernel,
        in_specs=[pl.BlockSpec(memory_space=pltpu.SMEM)] * 2 + [vmem] * 7,
        out_specs=[vmem] * 2,
        out_shape=[
            pltpu.VMEM((ROWS // 2, 80, 128), f32),
            pltpu.VMEM((ROWS // 2, 80, 128), bf16),
        ],
        scratch_shapes=[pltpu.VMEM((FAR, WIDE), bf16)],
        compiler_params=pltpu.CompilerParams(vmem_limit_bytes=20 << 20),
        name="finish_far",
    )(x, core, left, one, two, inverse, total, squares, column)


def other_core(array):
    return lax.ppermute(array, C, [(0, 1), (1, 0)])


def step_by(array, shift):
    n = lax.axis_size(X)
    return lax.ppermute(array, X, [(i, (i + shift) % n) for i in range(n)])


def pair_kernel(keep_ref, came_ref, out_ref):
    total = keep_ref[...] + came_ref[...].astype(f32)
    noise = jnp.sum(total[:, SITES:24], axis=1, keepdims=True)
    row = lax.broadcasted_iota(jnp.int32, total.shape, 1)
    for n, part in enumerate(three(noise)):
        total = jnp.where(row == SITES + n, part, total)
    out_ref[...] = total.astype(bf16)


def pair_of(keep, came):
    vmem = pl.BlockSpec(memory_space=pltpu.VMEM)
    return pl.pallas_call(
        pair_kernel,
        in_specs=[vmem] * 2,
        out_specs=vmem,
        out_shape=pltpu.VMEM(came.shape, bf16),
        compiler_params=pltpu.CompilerParams(vmem_limit_bytes=8 << 20),
        name="pair",
    )(keep, came)


def unpack(piece):
    ends = piece[:, 72:]
    ends = [ends] + [pltpu.roll(ends, 128 - REST * n, 2) for n in (1, 2)]
    tiles = [piece[:, 24 * n : 24 * n + 24] for n in range(3)]
    return jnp.concatenate(tiles + [jnp.concatenate(ends, axis=1)], axis=2)


def merge_kernel(core_ref, mine_ref, theirs_ref, out_ref, low_ref, high_ref):
    second = core_ref[0] == 1
    mine, theirs = mine_ref[...].astype(f32), theirs_ref[...].astype(f32)
    low_ref[...] = unpack(jnp.where(second, theirs, mine))
    high_ref[...] = unpack(jnp.where(second, mine, theirs))
    for q in range(SITES):
        rows = jnp.concatenate([low_ref[:, q, :], high_ref[:, q, :]], axis=0)
        out_ref[q] = rows[:, :STEPS].astype(bf16)


def merge(core, mine, theirs):
    vmem = pl.BlockSpec(memory_space=pltpu.VMEM)
    return pl.pallas_call(
        merge_kernel,
        in_specs=[pl.BlockSpec(memory_space=pltpu.SMEM)] + [vmem] * 2,
        out_specs=vmem,
        out_shape=jax.ShapeDtypeStruct((SITES, ROWS, STEPS), bf16),
        scratch_shapes=[pltpu.VMEM((ROWS // 2, 24, WIDE), f32)] * 2,
        compiler_params=pltpu.CompilerParams(vmem_limit_bytes=8 << 20),
        name="merge",
    )(core, mine, theirs)


def total_kernel(got_ref, rep_ref, noise_ref):
    total = jnp.sum(got_ref[...].astype(f32), axis=0)
    rep_ref[...] = jnp.broadcast_to(total.astype(bf16)[None], rep_ref.shape)
    tail = total[16:24, :SITES]
    row = lax.broadcasted_iota(jnp.int32, tail.shape, 0)
    noise_ref[...] = jnp.sum(jnp.where(row >= SITES - 16, tail, 0.0), axis=0, keepdims=True)


def total_of(got):
    vmem = pl.BlockSpec(memory_space=pltpu.VMEM)
    return pl.pallas_call(
        total_kernel,
        in_specs=[vmem],
        out_specs=[vmem] * 2,
        out_shape=[
            pltpu.VMEM(got.shape, bf16),
            jax.ShapeDtypeStruct((1, SITES), f32),
        ],
        compiler_params=pltpu.CompilerParams(vmem_limit_bytes=8 << 20),
        name="total",
    )(got)


def turn_kernel(bin_ref, lead_ref, raw_ref, rep_ref):
    w = raw_ref[...].astype(f32).reshape(HALVES, SLOTS, 128)
    lane = lax.broadcasted_iota(jnp.int32, (1, 128), 1)
    chunk = jnp.zeros((1, 128), jnp.int32)
    for g in range(1, CHUNKS):
        chunk += (lane >= SITES * g).astype(jnp.int32)
    lead = jnp.concatenate([lead_ref[...].astype(f32), jnp.zeros((1, 128 - SITES), f32)], axis=1)
    leads = lead
    for g in range(1, CHUNKS):
        leads = leads + pltpu.roll(lead, SITES * g, 1)
    outs = []
    for h in range(HALVES):
        half = HALVES * chunk + h
        real = half % 2 == 0
        turn = (bin_ref[0] + half // 2).astype(f32) * leads
        turn = turn - PERIOD * jnp.floor(turn * (1.0 / PERIOD))
        turn = jnp.where(turn < 0, turn + PERIOD, jnp.where(turn >= PERIOD, turn - PERIOD, turn))
        angle = turn * (2.0 * math.pi / PERIOD)
        cos, sin = jnp.cos(angle), jnp.sin(angle)
        above = w[h + 1] if h < HALVES - 1 else pltpu.roll(w[0], 128 - SITES, 1)
        below = w[h - 1] if h > 0 else pltpu.roll(w[HALVES - 1], SITES, 1)
        other = jnp.where(real, above, below)
        outs.append(w[h] * cos + other * jnp.where(real, -sin, sin))
    out = jnp.concatenate(outs, axis=0).astype(bf16)
    rep_ref[...] = jnp.broadcast_to(out[None], rep_ref.shape)


def copies_of(response, advance_offset, first_bin):
    half = response.reshape(2 * BINS, SLOTS, SITES)
    half = jnp.pad(half, ((0, CHUNKS * HALVES - 2 * BINS), (0, 0), (0, 0)))
    half = half.reshape(CHUNKS, DEPTH, SITES).transpose(1, 0, 2).reshape(DEPTH, CHUNKS * SITES)
    half = jnp.pad(half, ((0, 0), (0, 128 - CHUNKS * SITES)))
    vmem = pl.BlockSpec(memory_space=pltpu.VMEM)
    return pl.pallas_call(
        turn_kernel,
        in_specs=[pl.BlockSpec(memory_space=pltpu.SMEM)] + [vmem] * 2,
        out_specs=vmem,
        out_shape=pltpu.VMEM((8, DEPTH, 128), bf16),
        compiler_params=pltpu.CompilerParams(vmem_limit_bytes=8 << 20),
        name="turn",
    )(jnp.asarray(first_bin, jnp.int32).reshape(1), advance_offset.reshape(1, SITES), half)


def noise_of(slot_sensor, sensor_noise):
    ids = lax.iota(jnp.int32, sensor_noise.shape[0])
    slot_noise = jnp.sum(
        jnp.where(slot_sensor[:, None] == ids[None, :], sensor_noise[None, :], 0.0), axis=1
    )
    return slot_noise[:, None]


def on_device(samples, response, slot_sensor, sensor_noise, advance_offset):
    first_bin = lax.axis_index(FREQ) * BINS
    copies = copies_of(response, advance_offset, first_bin)
    x = lax.axis_index(X).astype(jnp.int32).reshape(1)
    core = lax.axis_index(C).astype(jnp.int32).reshape(1)
    copies, x, core = lax.optimization_barrier((copies, x, core))
    own, slot_sensor, sensor_noise = lax.optimization_barrier(
        (lax.all_to_all(copies, Z, 0, 0, tiled=True), slot_sensor, sensor_noise)
    )
    live = (slot_sensor >= 0).astype(bf16)[:, None]
    left, inverse, column = spread(samples, live, noise_of(slot_sensor, sensor_noise))
    prev, after = step_by(own, 1), step_by(own, -1)
    prev, after, left, inverse, column = lax.optimization_barrier(
        (prev, after, left, inverse, column)
    )
    total, squares = near(x, left, own, prev, after, inverse)
    one, two = step_by(prev[:4], 1), step_by(after[4:], -1)
    keep, send = finish_far(x, core, left, one, two, inverse, total, squares, column)
    got = lax.all_to_all(pair_of(keep, other_core(send)), Y, 0, 0, tiled=True)
    copies, noise = total_of(got)
    copies, noise = lax.optimization_barrier((copies, noise.reshape(SITES)))
    mine = lax.all_to_all(copies, Y, 0, 0, tiled=True)
    theirs = other_core(mine)
    outlook = merge(core, mine, theirs).transpose(1, 0, 2)
    return outlook, noise


def solution(mesh):
    torus = Mesh(mesh.devices.reshape(4, 8, 8, 2), (X, Z, Y, C))
    return jax.shard_map(
        on_device,
        mesh=torus,
        in_specs=(P(FREQ, SENS, None), P(FREQ, None, SENS, None), P(SENS), P(), P()),
        out_specs=(P(FREQ, None, None), P()),
        check_vma=False,
    )
```
